32 devices in a mesh: tp: 4 (over z), dp: 8 (over y, x, core).
Axes of the slice: x: 2, y: 2, z: 4, core: 2. Of those that a mesh axis runs over, the one named last changes fastest.
Arguments:
- hidden_in: bfloat16 [16384, 1024], P('dp')
- targets: bfloat16 [16384, 1024], P('dp')
- w_up: bfloat16 [4, 1024, 4096], P(None, None, 'tp')
- w_down: bfloat16 [4, 4096, 1024], P(None, 'tp')
Outputs:
- output 1: float32 [4, 1024, 4096], P(None, None, 'tp')
- output 2: float32 [4, 4096, 1024], P(None, 'tp')
All inputs are finite; a program needn't handle non-finite values.
Results may differ from the reference program's by a relative error of at most 0.0103568.
Values are sent between devices in bfloat16 or wider.
A program may use at most 1 GiB of HBM per device.

```python
import math
import jax
import jax.numpy as jnp
from jax import lax

D = 1024
FF = 4096
TOKENS = 16384
BLOCK_ROWS = 512
LAYERS = 4


def setup_inputs(seed: int = 0) -> dict:
    keys = jax.random.split(jax.random.key(seed), 4)
    tgt_scale = 2.0 * math.sqrt(TOKENS)
    hidden_in = jax.random.normal(keys[0], (TOKENS, D), jnp.float32)
    targets = tgt_scale * jax.random.normal(keys[1], (TOKENS, D), jnp.float32)
    w_up = jax.random.normal(keys[2], (LAYERS, D, FF), jnp.float32) * (D ** -0.5)
    w_down = jax.random.normal(keys[3], (LAYERS, FF, D), jnp.float32) * (FF ** -0.5)
    return {"hidden_in": hidden_in.astype(jnp.bfloat16), "targets": targets.astype(jnp.bfloat16), "w_up": w_up.astype(jnp.bfloat16), "w_down": w_down.astype(jnp.bfloat16)}


def gelu_tanh(value):
    return jax.nn.gelu(value, approximate=True)


def block_grads(hidden, target, w_up, w_down):
    def fwd_layer(h_cur, weights):
        up_w, down_w = weights
        pre_act = jnp.dot(h_cur, up_w, preferred_element_type=jnp.float32).astype(jnp.bfloat16)
        act_val = gelu_tanh(pre_act.astype(jnp.float32)).astype(jnp.bfloat16)
        branch = jnp.dot(act_val, down_w, preferred_element_type=jnp.float32).astype(jnp.bfloat16)
        return h_cur + branch, (h_cur, pre_act, act_val)

    h_last, saved = lax.scan(fwd_layer, hidden, (w_up, w_down))
    err_f32 = (h_last.astype(jnp.float32) - target.astype(jnp.float32)) / TOKENS

    def bwd_layer(g_cur, layer_in):
        h_in, pre_act, act_val, up_w, down_w = layer_in
        g_down = jnp.dot(act_val.T, g_cur, preferred_element_type=jnp.float32)
        d_act = jnp.dot(g_cur, down_w.T, preferred_element_type=jnp.float32)
        _, gelu_vjp = jax.vjp(gelu_tanh, pre_act.astype(jnp.float32))
        d_pre = gelu_vjp(d_act)[0].astype(jnp.bfloat16)
        g_up = jnp.dot(h_in.T, d_pre, preferred_element_type=jnp.float32)
        back_sum = g_cur.astype(jnp.float32) + jnp.dot(d_pre, up_w.T, preferred_element_type=jnp.float32)
        return back_sum.astype(jnp.bfloat16), (g_up, g_down)

    _, grads = lax.scan(bwd_layer, err_f32.astype(jnp.bfloat16), (saved[0], saved[1], saved[2], w_up, w_down), reverse=True)
    return grads


def reference(hidden_in, targets, w_up, w_down):
    num_blocks = TOKENS // BLOCK_ROWS
    hid_blocks = hidden_in.reshape(num_blocks, BLOCK_ROWS, D)
    tgt_blocks = targets.reshape(num_blocks, BLOCK_ROWS, D)

    def accumulate(acc_grads, block_pair):
        g_up, g_down = block_grads(block_pair[0], block_pair[1], w_up, w_down)
        return (acc_grads[0] + g_up, acc_grads[1] + g_down), None

    zero_grads = (jnp.zeros((LAYERS, D, FF), jnp.float32), jnp.zeros((LAYERS, FF, D), jnp.float32))
    (grad_up, grad_down), _ = lax.scan(accumulate, zero_grads, (hid_blocks, tgt_blocks))
    return grad_up, grad_down
```

```python
import functools
import math
import jax
import jax.numpy as jnp
from jax import lax
from jax.experimental import pallas as pl
from jax.experimental.pallas import tpu as pltpu
from jax.sharding import PartitionSpec as P

BF16 = jnp.bfloat16
F32 = jnp.float32
MESH = pl.DeviceIdType.MESH
TILES = 4
K0 = math.sqrt(2.0 / math.pi)
K1 = 0.044715 * K0
BY_ROWS = (((0,), (0,)), ((), ()))
BY_COLS = (((1,), (1,)), ((), ()))


def dot_cols(lhs, rhs):
    return lax.dot_general(lhs, rhs, BY_COLS, preferred_element_type=F32)


def dot_rows(lhs, rhs):
    return lax.dot_general(lhs, rhs, BY_ROWS, preferred_element_type=F32)


class Place:
    def __init__(self):
        z = lax.axis_index("tp")
        d = lax.axis_index("dp")
        self.core = lax.rem(d, 2)
        self.x = lax.rem(lax.div(d, 2), 2)
        self.y = lax.div(d, 4)
        self.across = {
            1: {"tp": z + 1 - 2 * lax.rem(z, 2)},
            2: {"tp": lax.rem(z + 2, 4)},
            3: {"tp": 3 - z},
        }
        self.x_dev = {"dp": self.index(self.y, 1 - self.x, self.core)}
        self.y_dev = {"dp": self.index(1 - self.y, self.x, self.core)}
        self.partner = {"dp": self.index(self.y, self.x, 1 - self.core)}

    @staticmethod
    def index(y, x, core):
        return y * 4 + x * 2 + core


def remote(src, dst, send_sem, recv_sem, device):
    return pltpu.make_async_remote_copy(src_ref=src, dst_ref=dst, send_sem=send_sem, recv_sem=recv_sem, device_id=device, device_id_type=MESH)


def meet(devices):
    barrier = pltpu.get_barrier_semaphore()
    for device in devices:
        pl.semaphore_signal(barrier, inc=1, device_id=device, device_id_type=MESH)
    pl.semaphore_wait(barrier, len(devices))


def forward_kernel(
    layers, total, x_ref, t_ref, up_ref, down_ref, w_ref, u_ref, a_ref, h_ref, g_ref,
    h_v, y_v, t_v, w_v, u_v, a_v, w_sem, u_sem, a_sem, h_sem, t_sem,
    zs, zr, xs, xr, ys, yr, as_, ar, bs, br, ds, dr,
):
    me = Place()
    groups = 3 * layers
    m, d = h_v.shape
    tm = m // TILES
    part = d // 8
    half = part // 2
    meet([me.across[1], me.across[2], me.across[3], me.x_dev, me.y_dev, me.partner])

    def rows(y, x):
        return pl.multiple_of(me.core * (4 * part) + (y * 2 + x) * part, part)

    mine, of_x, of_y, of_d = rows(me.y, me.x), rows(me.y, 1 - me.x), rows(1 - me.y, me.x), rows(1 - me.y, 1 - me.x)
    half_mine = pl.multiple_of(me.core * (4 * part), 4 * part)
    half_other = pl.multiple_of((1 - me.core) * (4 * part), 4 * part)

    def piece(c, start, size):
        return w_ref.at[c, :, pl.ds(start, size), :]

    def z_copy(c, s):
        return remote(piece(c, mine, part), piece(c, mine, part), zs.at[c], zr.at[c], me.across[s])

    def x_copy(c, start):
        return remote(piece(c, start, part), piece(c, start, part), xs.at[c], xr.at[c], me.x_dev)

    def y_copy(c, start):
        return remote(piece(c, start, part), piece(c, start, part), ys.at[c], yr.at[c], me.y_dev)

    def a_copy(c, start):
        return remote(piece(c, start, half), piece(c, start, half), as_.at[c], ar.at[c], me.y_dev)

    def b_copy(c, start):
        return remote(piece(c, start + half, half), piece(c, start + half, half), bs.at[c], br.at[c], me.x_dev)

    def d_copy(c, start):
        return remote(piece(c, start, 4 * part), piece(c, start, 4 * part), ds.at[c], dr.at[c], me.partner)

    def fetch_layer(l):
        for s in (1, 2, 3):
            c = 3 * l + s - 1
            for k, own in enumerate((up_ref, down_ref)):
                remote(own.at[l, pl.ds(mine, part), :], w_ref.at[c, k, pl.ds(mine, part), :], zs.at[c], zr.at[c], me.across[s]).start()

    def stage1(c):
        z_copy(c, 1).wait_recv()
        x_copy(c, mine).start()
        y_copy(c, mine).start()

    def stage2(c):
        x_copy(c, of_x).wait_recv()
        a_copy(c, of_x).start()
        y_copy(c, of_y).wait_recv()
        b_copy(c, of_y).start()

    def stage3(c):
        a_copy(c, of_d).wait_recv()
        b_copy(c, of_d).wait_recv()
        d_copy(c, half_mine).start()

    fetch_layer(0)
    fetch_layer(1)
    first = pltpu.make_async_copy(x_ref, h_v, t_sem.at[0])
    first.start()
    last = pltpu.make_async_copy(t_ref, t_v, t_sem.at[1])
    last.start()
    y_v[...] = jnp.zeros_like(y_v)
    first.wait()
    last.wait()

    def u_copy(it, t, slot):
        return pltpu.make_async_copy(u_v.at[slot], u_ref.at[it, pl.ds(t * tm, tm), :], u_sem.at[slot])

    def a_out(l, t, slot):
        return pltpu.make_async_copy(a_v.at[slot], a_ref.at[l, pl.ds(t * tm, tm), :], a_sem.at[slot])

    def h_out(dst, t):
        return pltpu.make_async_copy(h_v.at[pl.ds(t * tm, tm), :], dst.at[pl.ds(t * tm, tm), :], h_sem.at[t])

    def group(it, carry):
        l, s = lax.div(it, 4), lax.rem(it, 4)
        c = 3 * l + s - 1

        @pl.when((s == 0) & (l + 2 < layers))
        def _():
            fetch_layer(l + 2)

        @pl.when((s > 0) & (c + 1 < groups))
        def _():
            stage2(c + 1)

        @pl.when(s == 0)
        def _():
            pltpu.make_async_copy(up_ref.at[l], w_v.at[0], w_sem.at[0]).start()
            pltpu.make_async_copy(down_ref.at[l], w_v.at[1], w_sem.at[1]).start()

        @pl.when(s > 0)
        def _():
            d_copy(c, half_other).wait_recv()
            pltpu.make_async_copy(w_ref.at[c, 0], w_v.at[0], w_sem.at[0]).start()
            pltpu.make_async_copy(w_ref.at[c, 1], w_v.at[1], w_sem.at[1]).start()

        for k in (0, 1):
            pltpu.make_async_copy(up_ref.at[l], w_v.at[k], w_sem.at[k]).wait()

        def tile(t, carry):
            n = it * TILES + t
            slot = lax.rem(t, 2)
            here = pl.ds(pl.multiple_of(t * tm, tm), tm)

            @pl.when(n >= 2)
            def _():
                u_copy(it, t, slot).wait()

            @pl.when((n >= 2) & (lax.rem(lax.div(n - 2, TILES), 4) == 0))
            def _():
                a_out(l, t, slot).wait()

            wide = min(256, d)
            for j in range(0, d, wide):
                u = jnp.dot(h_v[here, :], w_v[0, :, j:j + wide], preferred_element_type=F32).astype(BF16)
                u_v[slot, :, j:j + wide] = u
                v = u.astype(F32)
                th = jnp.tanh(v * (K0 + K1 * (v * v)))
                hv = 0.5 * v
                a_v[slot, :, j:j + wide] = (hv + hv * th).astype(BF16)
            u_copy(it, t, slot).start()

            @pl.when(s == 0)
            def _():
                a_out(l, t, slot).start()

            for j in range(0, d, wide):
                y_v[here, j:j + wide] += jnp.dot(a_v[slot], w_v[1, :, j:j + wide], preferred_element_type=F32)

            @pl.when(s == 3)
            def _():
                @pl.when(l > 0)
                def _():
                    h_out(g_ref, t).wait()

                h_new = (h_v[here, :].astype(F32) + y_v[here, :].astype(BF16).astype(F32)).astype(BF16)
                y_v[here, :] = jnp.zeros((tm, d), F32)

                @pl.when(l < layers - 1)
                def _():
                    h_v[here, :] = h_new
                    h_out(h_ref.at[l], t).start()

                @pl.when(l == layers - 1)
                def _():
                    h_v[here, :] = ((h_new.astype(F32) - t_v[here, :].astype(F32)) / total).astype(BF16)
                    h_out(g_ref, t).start()

            @pl.when((it == 0) & (t == 0))
            def _():
                stage1(0)

            @pl.when((it == 0) & (t == 1))
            def _():
                stage1(1)
                stage2(0)

            @pl.when((it == 0) & (t == 3))
            def _():
                stage3(0)

            @pl.when((s > 0) & (t == 0) & (c + 2 < groups))
            def _():
                stage1(c + 2)

            @pl.when((s > 0) & (t == 2) & (c + 1 < groups))
            def _():
                stage3(c + 1)

            return carry

        lax.fori_loop(0, TILES, tile, 0)
        return carry

    lax.fori_loop(0, 4 * layers, group, 0)
    for slot in (0, 1):
        u_copy(0, slot, slot).wait()
    for t in range(TILES):
        h_out(g_ref, t).wait()

    def drain(c, carry):
        z_copy(c, 1).wait_send()
        x_copy(c, mine).wait_send()
        y_copy(c, mine).wait_send()
        a_copy(c, of_x).wait_send()
        b_copy(c, of_y).wait_send()
        d_copy(c, half_mine).wait_send()
        return carry

    lax.fori_loop(0, groups, drain, 0)


def backward_kernel(
    layers, x_ref, h_ref, up_ref, down_ref, w_ref, u_ref, a_ref, g_ref, gu_ref, gd_ref,
    g_v, acc_v, w_v, u_v, d_v, a_v, h_v, sums, in1, in2, in3, w_sem, u_sem, a_sem, h_sem, g_sem, out_sem, free1,
    s1, r1, s2, r2, s3, r3, s4, r4, s5, r5, s6, r6,
):
    me = Place()
    m, d = g_v.shape
    tm = m // TILES
    hd, qd = d // 2, d // 4
    e8, e16 = d // 8, d // 16
    wide = min(256, d)
    chunks = d // wide
    meet([me.x_dev, me.y_dev, me.partner])

    def at(value, size):
        return pl.ds(pl.multiple_of(value, size), size)

    own = me.core * hd
    own_rows, other_rows = at(own, hd), at(hd - own, hd)
    a_base, b_base = own, own + qd
    a_keep, a_give = at(a_base + me.x * e8, e8), at(a_base + (1 - me.x) * e8, e8)
    b_keep, b_give = at(b_base + me.y * e8, e8), at(b_base + (1 - me.y) * e8, e8)
    a_last, a_pass = at(a_base + me.x * e8 + me.y * e16, e16), at(a_base + me.x * e8 + (1 - me.y) * e16, e16)
    b_last, b_pass = at(b_base + me.y * e8 + me.x * e16, e16), at(b_base + me.y * e8 + (1 - me.x) * e16, e16)

    def c1(j):
        return remote(sums.at[lax.rem(j, 4), other_rows, :], in1.at[lax.rem(j, 2)], s1.at[j], r1.at[j], me.partner)

    def c2(j):
        q, r = lax.rem(j, 4), lax.rem(j, 2)
        return (remote(sums.at[q, a_give, :], in2.at[r, 0], s2.at[0, j], r2.at[0, j], me.x_dev),
                remote(sums.at[q, b_give, :], in2.at[r, 1], s2.at[1, j], r2.at[1, j], me.y_dev))

    def c3(j):
        q, r = lax.rem(j, 4), lax.rem(j, 2)
        return (remote(sums.at[q, a_pass, :], in3.at[r, 0], s3.at[0, j], r3.at[0, j], me.y_dev),
                remote(sums.at[q, b_pass, :], in3.at[r, 1], s3.at[1, j], r3.at[1, j], me.x_dev))

    def c4(j, ref, a_rows, b_rows):
        q, dst = lax.rem(j, 4), ref.at[layers - 1 - lax.div(j, 2)]
        return (remote(sums.at[q, a_rows, :], dst.at[a_rows, :], s4.at[0, j], r4.at[0, j], me.y_dev),
                remote(sums.at[q, b_rows, :], dst.at[b_rows, :], s4.at[1, j], r4.at[1, j], me.x_dev))

    def keep(j, ref):
        q, dst = lax.rem(j, 4), ref.at[layers - 1 - lax.div(j, 2)]
        return (pltpu.make_async_copy(sums.at[q, a_last, :], dst.at[a_last, :], out_sem.at[0, lax.rem(j, 2)]),
                pltpu.make_async_copy(sums.at[q, b_last, :], dst.at[b_last, :], out_sem.at[1, lax.rem(j, 2)]))

    def c5(j, ref, a_rows, b_rows):
        dst = ref.at[layers - 1 - lax.div(j, 2)]
        return (remote(dst.at[a_rows, :], dst.at[a_rows, :], s5.at[0, j], r5.at[0, j], me.x_dev),
                remote(dst.at[b_rows, :], dst.at[b_rows, :], s5.at[1, j], r5.at[1, j], me.y_dev))

    def c6(j, ref, which):
        dst = ref.at[layers - 1 - lax.div(j, 2)]
        return remote(dst.at[which, :], dst.at[which, :], s6.at[j], r6.at[j], me.partner)

    def add(j, start, size, buffer):
        q = lax.rem(j, 4)
        step = min(32, size)

        def body(i, carry):
            there = pl.ds(pl.multiple_of(start + i * step, step), step)
            sums[q, there, :] = sums[q, there, :] + buffer[pl.ds(pl.multiple_of(i * step, step), step), :]
            return carry

        lax.fori_loop(0, size // step, body, 0)

    def step1(j):
        @pl.when(j >= 2)
        def _():
            pl.semaphore_wait(free1, 1)

        c1(j).start()

    def step2(j):
        c1(j).wait_recv()
        add(j, own, hd, in1.at[lax.rem(j, 2)])

        @pl.when(j < 2 * layers - 2)
        def _():
            pl.semaphore_signal(free1, inc=1, device_id=me.partner, device_id_type=MESH)

        for copy in c2(j):
            copy.start()

    def step3(j):
        r, got, put = lax.rem(j, 2), c2(j), c3(j)
        for k, start in enumerate((a_base + me.x * e8, b_base + me.y * e8)):
            got[k].wait_recv()
            add(j, start, e8, in2.at[r, k])
            put[k].start()

    def step4(j, ref):
        r, got, put, local = lax.rem(j, 2), c3(j), c4(j, ref, a_last, b_last), keep(j, ref)
        for k, start in enumerate((a_base + me.x * e8 + me.y * e16, b_base + me.y * e8 + me.x * e16)):
            got[k].wait_recv()
            add(j, start, e16, in3.at[r, k])
            put[k].start()
            local[k].start()

    def step5(j, ref):
        got, put, local = c4(j, ref, a_pass, b_pass), c5(j, ref, a_keep, b_keep), keep(j, ref)
        for k in (0, 1):
            local[k].wait()
            got[k].wait_recv()
            put[k].start()

    def step6(j, ref):
        for copy in c5(j, ref, a_give, b_give):
            copy.wait_recv()
        c6(j, ref, own_rows).start()

    def step7(j, ref):
        c6(j, ref, other_rows).wait_recv()

    def settle(j, ref):
        c1(j).wait_send()
        for copy in c2(j) + c3(j) + c4(j, ref, a_last, b_last):
            copy.wait_send()

    def finish(j, ref):
        for copy in c5(j, ref, a_keep, b_keep):
            copy.wait_send()
        c6(j, ref, own_rows).wait_send()

    def u_copy(n):
        l, s, t = layers - 1 - lax.div(n, 16), lax.rem(lax.div(n, 4), 4), lax.rem(n, 4)
        slot = lax.rem(n, 2)
        return pltpu.make_async_copy(u_ref.at[4 * l + s, pl.ds(t * tm, tm), :], u_v.at[slot], u_sem.at[slot])

    def load_h(l):
        @pl.when(l == 0)
        def _():
            pltpu.make_async_copy(x_ref, h_v, h_sem).start()

        @pl.when(l > 0)
        def _():
            pltpu.make_async_copy(h_ref.at[l - 1], h_v, h_sem).start()

    def load_a(l):
        return pltpu.make_async_copy(a_ref.at[l], a_v, a_sem)

    def load_w(l, s):
        @pl.when(s == 0)
        def _():
            pltpu.make_async_copy(up_ref.at[l], w_v.at[0], w_sem.at[0]).start()
            pltpu.make_async_copy(down_ref.at[l], w_v.at[1], w_sem.at[1]).start()

        @pl.when(s > 0)
        def _():
            c = 3 * l + s - 1
            pltpu.make_async_copy(w_ref.at[c, 0], w_v.at[0], w_sem.at[0]).start()
            pltpu.make_async_copy(w_ref.at[c, 1], w_v.at[1], w_sem.at[1]).start()

    tiles_total = 16 * (layers - 1) + 4
    start_g = pltpu.make_async_copy(g_ref, g_v, g_sem)
    start_g.start()
    load_a(layers - 1).start()
    load_h(layers - 1)
    u_copy(0).start()
    start_g.wait()

    def layer(tau, carry):
        l = layers - 1 - tau
        down, up = 2 * tau, 2 * tau + 1
        qd_, qu_ = lax.rem(down, 4), lax.rem(up, 4)
        later = tau > 0
        load_w(l, 0)
        load_a(l).wait()

        @pl.when(tau >= 2)
        def _():
            settle(down - 4, gd_ref)

        def down_chunk(i, carry):
            k = lax.rem(i + (1 - me.core) * (chunks // 2), chunks)
            cols = pl.ds(pl.multiple_of(k * wide, wide), wide)
            sums[qd_, cols, :] = dot_rows(a_v[:, cols], g_v[...])

            @pl.when(i == chunks // 2 - 1)
            def _():
                step1(down)

                @pl.when(later)
                def _():
                    step5(down - 2, gd_ref)

            return carry

        lax.fori_loop(0, chunks, down_chunk, 0)

        @pl.when(l > 0)
        def _():
            load_a(l - 1).start()

        def block(s, carry):
            @pl.when(s > 0)
            def _():
                load_w(l, s)

            for k in (0, 1):
                pltpu.make_async_copy(up_ref.at[l], w_v.at[k], w_sem.at[k]).wait()

            def tile(t, carry):
                n = 16 * tau + 4 * s + t
                slot = lax.rem(n, 2)
                here = pl.ds(pl.multiple_of(t * tm, tm), tm)

                @pl.when(n + 1 < tiles_total)
                def _():
                    u_copy(n + 1).start()

                u_copy(n).wait()
                for j in range(0, d, wide):
                    da = dot_cols(g_v[here, :], w_v[1, j:j + wide, :])
                    v = u_v[slot, :, j:j + wide].astype(F32)
                    v2 = v * v
                    th = jnp.tanh(v * (K0 + K1 * v2))
                    slope = (0.5 + 0.5 * th) + (0.5 * v) * (1.0 - th * th) * (K0 + (3.0 * K1) * v2)
                    d_v[here, j:j + wide] = (da * slope).astype(BF16)

                @pl.when((l > 0) & (s == 0))
                def _():
                    for j in range(0, d, wide):
                        acc_v[here, j:j + wide] = g_v[here, j:j + wide].astype(F32) + dot_cols(d_v[here, :], w_v[0, j:j + wide, :])

                @pl.when((s > 0) & (s < 3))
                def _():
                    for j in range(0, d, wide):
                        acc_v[here, j:j + wide] += dot_cols(d_v[here, :], w_v[0, j:j + wide, :])

                @pl.when(s == 3)
                def _():
                    for j in range(0, d, wide):
                        total = acc_v[here, j:j + wide] + dot_cols(d_v[here, :], w_v[0, j:j + wide, :])
                        g_v[here, j:j + wide] = total.astype(BF16)

                def when(cond, run):
                    @pl.when(cond)
                    def _():
                        run()

                when((s == 0) & (t == 0), lambda: step2(down))
                when((s == 0) & (t == 1) & later, lambda: step4(down - 1, gu_ref))
                when((s == 0) & (t == 2) & later, lambda: step6(down - 2, gd_ref))
                when((s == 1) & (t == 1) & later, lambda: step5(down - 1, gu_ref))
                when((s == 1) & (t == 3), lambda: step2(up))
                when((s == 2) & (t == 0), lambda: step4(down, gd_ref))
                when((s == 2) & (t == 1) & later, lambda: step6(down - 1, gu_ref))
                when((s == 3) & (t == 0) & later, lambda: step7(down - 1, gu_ref))
                when((s == 3) & (t == 3), lambda: step3(up))
                return carry

            lax.fori_loop(0, TILES, tile, 0)

            @pl.when(s == 0)
            def _():
                pltpu.make_async_copy(x_ref, h_v, h_sem).wait()

                @pl.when(tau >= 2)
                def _():
                    settle(up - 4, gu_ref)

                def up_chunk(i, carry):
                    k = lax.rem(i + (1 - me.core) * (chunks // 2), chunks)
                    cols = pl.ds(pl.multiple_of(k * wide, wide), wide)
                    sums[qu_, cols, :] = dot_rows(h_v[:, cols], d_v[...])

                    @pl.when(i == chunks // 2 - 1)
                    def _():
                        step1(up)

                    return carry

                lax.fori_loop(0, chunks, up_chunk, 0)

                @pl.when(l > 0)
                def _():
                    load_h(l - 1)

                @pl.when(later)
                def _():
                    step7(down - 2, gd_ref)

                step3(down)

            return carry

        lax.fori_loop(0, jnp.where(l > 0, 4, 1), block, 0)
        return carry

    lax.fori_loop(0, layers, layer, 0)
    down, up = 2 * layers - 2, 2 * layers - 1
    step5(down - 1, gu_ref)
    step2(up)
    step4(down, gd_ref)
    step6(down - 1, gu_ref)
    step3(up)
    step7(down - 1, gu_ref)
    step5(down, gd_ref)
    step4(up, gu_ref)
    step6(down, gd_ref)
    step5(up, gu_ref)
    step7(down, gd_ref)
    step6(up, gu_ref)
    step7(up, gu_ref)

    def drain(tau, carry):
        finish(2 * tau, gd_ref)
        finish(2 * tau + 1, gu_ref)

        @pl.when(tau >= layers - 2)
        def _():
            settle(2 * tau, gd_ref)
            settle(2 * tau + 1, gu_ref)

        return carry

    lax.fori_loop(0, layers, drain, 0)


def any_specs(count):
    return [pl.BlockSpec(memory_space=pl.ANY)] * count


def local_step(hidden, targets, w_up, w_down, total_tokens):
    layers, d, own = w_up.shape
    m = hidden.shape[0]
    tm = m // TILES
    groups = 3 * layers
    dma = pltpu.SemaphoreType.DMA
    weights, acts, acts_own, states, g_last = pl.pallas_call(
        functools.partial(forward_kernel, layers, float(total_tokens)),
        out_shape=[
            jax.ShapeDtypeStruct((groups, 2, d, own), BF16),
            jax.ShapeDtypeStruct((4 * layers, m, own), BF16),
            jax.ShapeDtypeStruct((layers, m, own), BF16),
            jax.ShapeDtypeStruct((layers - 1, m, d), BF16),
            jax.ShapeDtypeStruct((m, d), BF16),
        ],
        in_specs=any_specs(4),
        out_specs=any_specs(5),
        scratch_shapes=[
            pltpu.VMEM((m, d), BF16),
            pltpu.VMEM((m, d), F32),
            pltpu.VMEM((m, d), BF16),
            pltpu.VMEM((2, d, own), BF16),
            pltpu.VMEM((2, tm, own), BF16),
            pltpu.VMEM((2, tm, own), BF16),
            dma((2,)), dma((2,)), dma((2,)), dma((TILES,)), dma((2,)),
        ] + [dma((groups,))] * 12,
        compiler_params=pltpu.CompilerParams(collective_id=0, has_side_effects=True, vmem_limit_bytes=60 << 20),
        name="forward",
    )(hidden, targets, w_up, w_down)
    grad_up, grad_down = pl.pallas_call(
        functools.partial(backward_kernel, layers),
        out_shape=[jax.ShapeDtypeStruct((layers, d, own), F32), jax.ShapeDtypeStruct((layers, own, d), F32)],
        in_specs=any_specs(8),
        out_specs=any_specs(2),
        scratch_shapes=[
            pltpu.VMEM((m, d), BF16),
            pltpu.VMEM((m, d), F32),
            pltpu.VMEM((2, d, own), BF16),
            pltpu.VMEM((2, tm, own), BF16),
            pltpu.VMEM((m, own), BF16),
            pltpu.VMEM((m, own), BF16),
            pltpu.VMEM((m, d), BF16),
            pltpu.VMEM((4, d, own), F32),
            pltpu.VMEM((2, d // 2, own), F32),
            pltpu.VMEM((2, 2, d // 8, own), F32),
            pltpu.VMEM((2, 2, d // 16, own), F32),
            dma((2,)), dma((2,)), dma, dma, dma, dma((2, 2)), pltpu.SemaphoreType.REGULAR,
            dma((2 * layers,)), dma((2 * layers,)),
        ] + [dma((2, 2 * layers))] * 8 + [dma((2 * layers,)), dma((2 * layers,))],
        compiler_params=pltpu.CompilerParams(collective_id=1, has_side_effects=True, vmem_limit_bytes=63 << 20),
        name="backward",
    )(hidden, states, w_up, w_down, weights, acts, acts_own, g_last)
    return grad_up, grad_down


def solution(mesh):
    def grad_step(hidden_in, targets, w_up, w_down):
        step_fn = functools.partial(local_step, total_tokens=hidden_in.shape[0])
        mapped = jax.shard_map(step_fn, mesh=mesh, in_specs=(P("dp", None), P("dp", None), P(None, None, "tp"), P(None, "tp", None)), out_specs=(P(None, None, "tp"), P(None, "tp", None)), check_vma=False)
        return mapped(hidden_in, targets, w_up, w_down)

    return grad_step
```

```python
import functools
import math
import jax
import jax.numpy as jnp
from jax import lax
from jax.experimental import pallas as pl
from jax.experimental.pallas import tpu as pltpu
from jax.sharding import PartitionSpec as P

BF16 = jnp.bfloat16
F32 = jnp.float32
MESH = pl.DeviceIdType.MESH
TILES = 4
K0 = math.sqrt(2.0 / math.pi)
K1 = 0.044715 * K0
BY_ROWS = (((0,), (0,)), ((), ()))
BY_COLS = (((1,), (1,)), ((), ()))


def dot_cols(lhs, rhs):
    return lax.dot_general(lhs, rhs, BY_COLS, preferred_element_type=F32)


def dot_rows(lhs, rhs):
    return lax.dot_general(lhs, rhs, BY_ROWS, preferred_element_type=F32)


class Place:
    def __init__(self):
        z = lax.axis_index("tp")
        d = lax.axis_index("dp")
        self.core = lax.rem(d, 2)
        self.x = lax.rem(lax.div(d, 2), 2)
        self.y = lax.div(d, 4)
        self.inner = (z == 1) | (z == 2)
        self.near = {"tp": z + 1 - 2 * lax.rem(z, 2)}
        self.middle = {"tp": 3 - z}
        self.x_dev = {"dp": self.index(self.y, 1 - self.x, self.core)}
        self.y_dev = {"dp": self.index(1 - self.y, self.x, self.core)}
        self.partner = {"dp": self.index(self.y, self.x, 1 - self.core)}

    @staticmethod
    def index(y, x, core):
        return y * 4 + x * 2 + core


def remote(src, dst, send_sem, recv_sem, device):
    return pltpu.make_async_remote_copy(src_ref=src, dst_ref=dst, send_sem=send_sem, recv_sem=recv_sem, device_id=device, device_id_type=MESH)


def meet(devices):
    barrier = pltpu.get_barrier_semaphore()
    for device in devices:
        pl.semaphore_signal(barrier, inc=1, device_id=device, device_id_type=MESH)
    pl.semaphore_wait(barrier, len(devices))


FORWARD_TIMES = {
    "F": (0, 0, 1, 3, 3, 6, 18, 16, 25, 29, 31, 36),
    "Z": (2, 5, 22),
    "1": (0, 0, 2, 5, 7, 12, 20, 20, 29, 33, 36, 44),
    "2": (2, 3, 4, 11, 14, 19, 25, 29, 35, 42, 45, 53),
    "3": (3, 6, 7, 15, 20, 24, 31, 33, 40, 47, 52, 56),
    "L": (3, 7, 10, 12, 18, 23, 26, 30, 33, 37, 42, 45, 49, 54, 58),
}

BACKWARD_TIMES = (
    (0, 6, 32, 38, 64, 70, 96, 102),
    (2, 8, 34, 40, 66, 72, 98, 128),
    (6, 12, 41, 44, 73, 76, 130, 131),
    (9, 16, 46, 47, 78, 79, 132, 133),
    (14, 32, 49, 51, 81, 83, 134, 135),
    (19, 37, 66, 69, 98, 103, 136, 138),
    (32, 39, 68, 71, 101, 129, 137, 139),
)


def forward_plan():
    events = []
    for rank, (kind, times) in enumerate(FORWARD_TIMES.items()):
        for i, n in enumerate(times):
            c = i + 1 if kind in "ZL" else i
            age = 3 * c - 2.5 if kind == "Z" else c if kind != "L" else 3 * (c // 4) + (c % 4 - 1 if c % 4 else -0.5)
            events.append((n, age, rank, kind, c))
    return [(n, kind, c) for n, _, _, kind, c in sorted(events)]


def backward_plan():
    return [(p, k, j) for p, j, k in sorted((p, j, k + 1) for k, times in enumerate(BACKWARD_TIMES) for j, p in enumerate(times))]


def at_step(plan, now, block, steps, run):
    for b in sorted({e[0] // block for e in plan}):
        here = [e for e in plan if e[0] // block == b and e[0] % block in steps]
        if not here:
            continue

        @pl.when(lax.div(now, block) == b)
        def _():
            for n in sorted({e[0] for e in here}):
                @pl.when(now == n)
                def _():
                    for e in here:
                        if e[0] == n:
                            run(e[1], e[2])


def forward_pass(
    layers, total, prefetch, x_ref, t_ref, up_ref, down_ref, w_ref, u_ref, a_ref, h_ref,
    h_v, y_v, t_v, w_v, u_v, a_v, w_sem, u_sem, a_sem, h_sem, t_sem,
    zs, zr, fs, xs, xr, ys, yr, as_, ar, bs, br, ds, dr,
):
    plan = forward_plan()
    me = Place()
    groups = 3 * layers
    m, d = h_v.shape
    tm = m // TILES
    part = d // 8
    half = part // 2
    last_n = 4 * TILES * layers - 1
    wide = min(256, d)

    def rows(y, x):
        return pl.multiple_of(me.core * (4 * part) + (y * 2 + x) * part, part)

    mine, of_x, of_y, of_d = rows(me.y, me.x), rows(me.y, 1 - me.x), rows(1 - me.y, me.x), rows(1 - me.y, 1 - me.x)
    half_mine = pl.multiple_of(me.core * (4 * part), 4 * part)
    half_other = pl.multiple_of((1 - me.core) * (4 * part), 4 * part)

    def piece(c, start, size):
        return w_ref.at[c, :, pl.ds(start, size), :]

    def z_copy(c):
        return remote(piece(c, mine, part), piece(c, mine, part), zs.at[c], zr.at[c], me.near)

    def f_copy(c):
        to, device = (c + 2, me.middle) if c % 3 == 0 else (c, me.near)
        return remote(piece(c, mine, part), piece(to, mine, part), fs.at[c], zr.at[to], device)

    def x_copy(c, start):
        return remote(piece(c, start, part), piece(c, start, part), xs.at[c], xr.at[c], me.x_dev)

    def y_copy(c, start):
        return remote(piece(c, start, part), piece(c, start, part), ys.at[c], yr.at[c], me.y_dev)

    def a_copy(c, start):
        return remote(piece(c, start, half), piece(c, start, half), as_.at[c], ar.at[c], me.y_dev)

    def b_copy(c, start):
        return remote(piece(c, start + half, half), piece(c, start + half, half), bs.at[c], br.at[c], me.x_dev)

    def d_copy(c, start):
        return remote(piece(c, start, 4 * part), piece(c, start, 4 * part), ds.at[c], dr.at[c], me.partner)

    def send_own(l, c, device):
        for k, own in enumerate((up_ref, down_ref)):
            remote(own.at[l, pl.ds(mine, part), :], w_ref.at[c, k, pl.ds(mine, part), :], zs.at[c], zr.at[c], device).start()

    def load_w(g):
        l, s, ws = g // 4, g % 4, g % 2
        c = 3 * l + s - 1
        if s > 0:
            d_copy(c, half_other).wait_recv()
        for k, own in enumerate((up_ref, down_ref)):
            pltpu.make_async_copy(own.at[l] if s == 0 else w_ref.at[c, k], w_v.at[ws, k], w_sem.at[ws, k]).start()

    def run(kind, c):
        if kind == "Z":
            send_own(c, 3 * c, me.near)

            @pl.when(me.inner)
            def _():
                send_own(c, 3 * c + 1, me.middle)
        elif kind == "F":
            @pl.when(me.inner)
            def _():
                z_copy(c).wait_recv()
                f_copy(c).start()
        elif kind == "1":
            @pl.when(jnp.logical_not(me.inner))
            def _():
                z_copy(c).wait_recv()

            x_copy(c, mine).start()
            y_copy(c, mine).start()
        elif kind == "2":
            x_copy(c, of_x).wait_recv()
            a_copy(c, of_x).start()
            y_copy(c, of_y).wait_recv()
            b_copy(c, of_y).start()
        elif kind == "3":
            a_copy(c, of_d).wait_recv()
            b_copy(c, of_d).wait_recv()
            d_copy(c, half_mine).start()
        else:
            load_w(c)

    first = pltpu.make_async_copy(x_ref, h_v, t_sem.at[0])
    first.start()
    load_w(0)
    meet([me.near, me.middle, me.x_dev, me.y_dev, me.partner])
    run("Z", 0)
    last = pltpu.make_async_copy(t_ref, t_v, t_sem.at[1])
    last.start()
    y_v[...] = jnp.zeros_like(y_v)
    first.wait()

    def tile_of(n):
        return lax.rem(n, TILES)

    def there(n):
        return pl.ds(pl.multiple_of(tile_of(n) * tm, tm), tm)

    def slot_of(n):
        return lax.rem(lax.div(n, TILES), 2)

    def wait_w(n):
        for k in (0, 1):
            pltpu.make_async_copy(up_ref.at[0], w_v.at[slot_of(n), k], w_sem.at[slot_of(n), k]).wait()

    def u_copy(n):
        slot = lax.rem(n, 2)
        return pltpu.make_async_copy(u_v.at[slot], u_ref.at[lax.div(n, TILES), there(n), :], u_sem.at[slot])

    def a_out(n):
        slot = lax.rem(n, 2)
        return pltpu.make_async_copy(a_v.at[slot], a_ref.at[lax.div(n, 4 * TILES), there(n), :], a_sem.at[slot])

    def h_out(dst, n):
        return pltpu.make_async_copy(h_v.at[there(n), :], dst.at[there(n), :], h_sem.at[tile_of(n)])

    def is_block(n, s):
        return lax.rem(lax.div(n, TILES), 4) == s

    def settle_rows(n):
        l = lax.div(n, 4 * TILES)

        @pl.when(l > 0)
        def _():
            h_out(h_ref.at[0], n).wait()

        def sweep(last_layer):
            size = min(32, tm)

            def body(i, carry):
                few = pl.ds(pl.multiple_of(tile_of(n) * tm + i * size, size), size)
                h_new = (h_v[few, :].astype(F32) + y_v[few, :].astype(BF16).astype(F32)).astype(BF16)
                if last_layer:
                    h_new = ((h_new.astype(F32) - t_v[few, :].astype(F32)) / total).astype(BF16)
                h_v[few, :] = h_new
                y_v[few, :] = h_new.astype(F32) if last_layer else jnp.zeros((size, d), F32)
                return carry

            lax.fori_loop(0, tm // size, body, 0)

        @pl.when(l < layers - 1)
        def _():
            sweep(False)
            h_out(h_ref.at[l], n).start()

        @pl.when(l == layers - 1)
        def _():
            sweep(True)

    def step(n, carry):
        here, slot, ws = there(n), lax.rem(n, 2), slot_of(n)

        @pl.when(n >= 2)
        def _():
            u_copy(n).wait()

        @pl.when((n >= 2) & is_block(n - 2, 0))
        def _():
            a_out(n).wait()

        @pl.when(tile_of(n) == 0)
        def _():
            wait_w(n)

        for j in range(0, d, wide):
            u = jnp.dot(h_v[here, :], w_v[ws, 0, :, j:j + wide], preferred_element_type=F32).astype(BF16)
            u_v[slot, :, j:j + wide] = u
            v = u.astype(F32)
            th = jnp.tanh(v * (K0 + K1 * (v * v)))
            hv = 0.5 * v
            a_v[slot, :, j:j + wide] = (hv + hv * th).astype(BF16)
        u_copy(n).start()

        @pl.when(is_block(n, 0))
        def _():
            a_out(n).start()

        @pl.when(n == last_n - TILES + 1)
        def _():
            prefetch()

        at_step(plan, n, 4 * TILES, range(4 * TILES), run)
        for j in range(0, d, wide):
            y_v[here, j:j + wide] += jnp.dot(a_v[slot], w_v[ws, 1, :, j:j + wide], preferred_element_type=F32)

        @pl.when(is_block(n, 3))
        def _():
            settle_rows(n)

        return carry

    last.wait()
    lax.fori_loop(0, last_n + 1, step, 0)
    u_copy(last_n - 1).wait()
    u_copy(last_n).wait()

    def drain():
        for c in range(groups):
            if c % 3 == 0:
                z_copy(c).wait_send()

            @pl.when(me.inner)
            def _():
                f_copy(c).wait_send()
                if c % 3 == 1:
                    z_copy(c).wait_send()

            x_copy(c, mine).wait_send()
            y_copy(c, mine).wait_send()
            a_copy(c, of_x).wait_send()
            b_copy(c, of_y).wait_send()
            d_copy(c, half_mine).wait_send()

    return drain


def backward_pass(
    layers, load_a, load_w, x_ref, h_ref, up_ref, u_ref, gu_ref, gd_ref,
    g_v, acc_v, w_v, u_v, d_v, a_v, h_v, sums, in1, in2, in3,
    w_sem, u_sem, h_sem, out_sem, free1,
    s1, r1, s2, r2, s3, r3, s4, r4, s5, r5, s6, r6,
):
    plan = backward_plan()
    me = Place()
    m, d = g_v.shape
    tm = m // TILES
    hd, qd = d // 2, d // 4
    e8, e16 = d // 8, d // 16
    wide = min(256, d)
    broad = d // 2

    def at(value, size):
        return pl.ds(pl.multiple_of(value, size), size)

    own = me.core * hd
    own_rows, other_rows = at(own, hd), at(hd - own, hd)
    a_base, b_base = own, own + qd
    a_keep, a_give = at(a_base + me.x * e8, e8), at(a_base + (1 - me.x) * e8, e8)
    b_keep, b_give = at(b_base + me.y * e8, e8), at(b_base + (1 - me.y) * e8, e8)
    a_last, a_pass = at(a_base + me.x * e8 + me.y * e16, e16), at(a_base + me.x * e8 + (1 - me.y) * e16, e16)
    b_last, b_pass = at(b_base + me.y * e8 + me.x * e16, e16), at(b_base + me.y * e8 + (1 - me.x) * e16, e16)

    def room(j):
        return lax.rem(j, 2) * (1 + lax.rem(lax.div(j, 2), 2))

    def c1(j):
        return remote(sums.at[room(j), other_rows, :], in1.at[lax.rem(j, 2)], s1.at[j], r1.at[j], me.partner)

    def c2(j):
        q, r = room(j), lax.rem(j, 2)
        return (remote(sums.at[q, a_give, :], in2.at[r, 0], s2.at[0, j], r2.at[0, j], me.x_dev),
                remote(sums.at[q, b_give, :], in2.at[r, 1], s2.at[1, j], r2.at[1, j], me.y_dev))

    def c3(j):
        q, r = room(j), lax.rem(j, 2)
        return (remote(sums.at[q, a_pass, :], in3.at[r, 0], s3.at[0, j], r3.at[0, j], me.y_dev),
                remote(sums.at[q, b_pass, :], in3.at[r, 1], s3.at[1, j], r3.at[1, j], me.x_dev))

    def c4(j, ref, a_rows, b_rows):
        q, dst = room(j), ref.at[layers - 1 - lax.div(j, 2)]
        return (remote(sums.at[q, a_rows, :], dst.at[a_rows, :], s4.at[0, j], r4.at[0, j], me.y_dev),
                remote(sums.at[q, b_rows, :], dst.at[b_rows, :], s4.at[1, j], r4.at[1, j], me.x_dev))

    def keep(j, ref):
        q, dst = room(j), ref.at[layers - 1 - lax.div(j, 2)]
        return (pltpu.make_async_copy(sums.at[q, a_last, :], dst.at[a_last, :], out_sem.at[0, lax.rem(j, 2)]),
                pltpu.make_async_copy(sums.at[q, b_last, :], dst.at[b_last, :], out_sem.at[1, lax.rem(j, 2)]))

    def c5(j, ref, a_rows, b_rows):
        dst = ref.at[layers - 1 - lax.div(j, 2)]
        return (remote(dst.at[a_rows, :], dst.at[a_rows, :], s5.at[0, j], r5.at[0, j], me.x_dev),
                remote(dst.at[b_rows, :], dst.at[b_rows, :], s5.at[1, j], r5.at[1, j], me.y_dev))

    def c6(j, ref, which):
        dst = ref.at[layers - 1 - lax.div(j, 2)]
        return remote(dst.at[which, :], dst.at[which, :], s6.at[j], r6.at[j], me.partner)

    def add(j, start, size, buffer):
        q = room(j)
        step = min(32, size)

        def body(i, carry):
            there = pl.ds(pl.multiple_of(start + i * step, step), step)
            sums[q, there, :] = sums[q, there, :] + buffer[pl.ds(pl.multiple_of(i * step, step), step), :]
            return carry

        lax.fori_loop(0, size // step, body, 0)

    def step1(j):
        @pl.when(j >= 2)
        def _():
            pl.semaphore_wait(free1, 1)

        c1(j).start()

    def step2(j):
        c1(j).wait_recv()
        add(j, own, hd, in1.at[lax.rem(j, 2)])

        @pl.when(j < 2 * layers - 2)
        def _():
            pl.semaphore_signal(free1, inc=1, device_id=me.partner, device_id_type=MESH)

        for copy in c2(j):
            copy.start()

    def step3(j):
        r, got, put = lax.rem(j, 2), c2(j), c3(j)
        for k, start in enumerate((a_base + me.x * e8, b_base + me.y * e8)):
            got[k].wait_recv()
            add(j, start, e8, in2.at[r, k])
            put[k].start()

    def step4(j, ref):
        r, got, put, local = lax.rem(j, 2), c3(j), c4(j, ref, a_last, b_last), keep(j, ref)
        for k, start in enumerate((a_base + me.x * e8 + me.y * e16, b_base + me.y * e8 + me.x * e16)):
            got[k].wait_recv()
            add(j, start, e16, in3.at[r, k])
            put[k].start()
            local[k].start()

    def step5(j, ref):
        got, put, local = c4(j, ref, a_pass, b_pass), c5(j, ref, a_keep, b_keep), keep(j, ref)
        for k in (0, 1):
            local[k].wait()
            got[k].wait_recv()
            put[k].start()

    def step6(j, ref):
        for copy in c5(j, ref, a_give, b_give):
            copy.wait_recv()
        c6(j, ref, own_rows).start()

    def step7(j, ref):
        c6(j, ref, other_rows).wait_recv()

    def settle(j, ref):
        c1(j).wait_send()
        for copy in c2(j) + c3(j) + c4(j, ref, a_last, b_last):
            copy.wait_send()

    def finish(j, ref):
        for copy in c5(j, ref, a_keep, b_keep):
            copy.wait_send()
        c6(j, ref, own_rows).wait_send()

    def run(k, j):
        ref = gd_ref if j % 2 == 0 else gu_ref
        (step1, step2, step3, step4, step5, step6, step7)[k - 1](*((j,) if k <= 3 else (j, ref)))

    def at_place(tau, p, steps):
        at_step(plan, 32 * tau + p, 32, steps, run)

    def u_copy(n):
        l, s, t, slot = layers - 1 - lax.div(n, 16), lax.rem(lax.div(n, 4), 4), lax.rem(n, 4), lax.rem(n, 2)
        return pltpu.make_async_copy(u_ref.at[4 * l + s, pl.ds(t * tm, tm), :], u_v.at[slot], u_sem.at[slot])

    def load_h(l):
        @pl.when(l == 0)
        def _():
            pltpu.make_async_copy(x_ref, h_v, h_sem).start()

        @pl.when(l > 0)
        def _():
            pltpu.make_async_copy(h_ref.at[l - 1], h_v, h_sem).start()

    def wait_w(i):
        for k in (0, 1):
            pltpu.make_async_copy(up_ref.at[0], w_v.at[lax.rem(i, 2), k], w_sem.at[lax.rem(i, 2), k]).wait()

    def next_g():
        step = min(64, m)

        def body(i, carry):
            here = pl.ds(pl.multiple_of(i * step, step), step)
            g_v[here, :] = acc_v[here, :].astype(BF16)
            acc_v[here, :] = g_v[here, :].astype(F32)
            return carry

        lax.fori_loop(0, m // step, body, 0)

    load_h(layers - 1)
    u_copy(0).start()
    tiles_total = 16 * (layers - 1) + 4
    groups = 4 * (layers - 1) + 1

    def layer(tau, carry):
        l = layers - 1 - tau
        down, up = 2 * tau, 2 * tau + 1
        room_down, room_up = room(down), room(up)
        load_a(l).wait()

        @pl.when(tau > 0)
        def _():
            settle(down - 2, gd_ref)

        def product(room_j, lhs, rhs, base):
            def body(i, carry):
                cols = at(lax.rem(i + 1 + me.core, 2) * broad, broad)
                sums[room_j, cols, :] = dot_rows(lhs[:, cols], rhs[...])
                at_place(tau, base + i, (base, base + 1))
                return carry

            lax.fori_loop(0, 2, body, 0)

        product(room_down, a_v, g_v, 0)

        @pl.when(l > 0)
        def _():
            load_a(l - 1).start()

        def step(n, carry):
            k = 16 * tau + n
            block, slot = 4 * tau + lax.div(n, TILES), lax.rem(k, 2)
            ws = lax.rem(block, 2)
            here = pl.ds(pl.multiple_of(lax.rem(n, TILES) * tm, tm), tm)

            @pl.when(k + 1 < tiles_total)
            def _():
                u_copy(k + 1).start()

            @pl.when(lax.rem(n, TILES) == 0)
            def _():
                @pl.when(block + 1 < groups)
                def _():
                    load_w(block + 1)

                wait_w(block)

            u_copy(k).wait()
            for j in range(0, d, wide):
                da = dot_cols(g_v[here, :], w_v[ws, 1, j:j + wide, :])
                v = u_v[slot, :, j:j + wide].astype(F32)
                v2 = v * v
                th = jnp.tanh(v * (K0 + K1 * v2))
                slope = (1.0 + th) * (0.5 + (v * (1.0 - th)) * ((0.5 * K0) + (1.5 * K1) * v2))
                d_v[here, j:j + wide] = (da * slope).astype(BF16)
            at_place(tau, n + jnp.where(n >= 4, 4, 2), list(range(2, 6)) + list(range(8, 20)))

            @pl.when(l > 0)
            def _():
                for j in range(0, d, wide):
                    acc_v[here, j:j + wide] += dot_cols(d_v[here, :], w_v[ws, 0, j:j + wide, :])

            @pl.when(n == TILES - 1)
            def _():
                pltpu.make_async_copy(x_ref, h_v, h_sem).wait()

                @pl.when(tau >= 2)
                def _():
                    settle(up - 4, gu_ref)

                product(room_up, h_v, d_v, 6)

                @pl.when(l > 0)
                def _():
                    load_h(l - 1)

            return carry

        lax.fori_loop(0, jnp.where(l > 0, 16, 4), step, 0)

        @pl.when(l > 0)
        def _():
            next_g()
            at_place(tau, 20, (20,))

        return carry

    lax.fori_loop(0, layers, layer, 0)
    for p, k, j in plan:
        if p >= 32 * layers:
            run(k, j)
    for j in range(2 * layers):
        ref = gd_ref if j % 2 == 0 else gu_ref
        finish(j, ref)
        if j >= 2 * layers - 3 and j != 2 * layers - 4:
            settle(j, ref)


def kernel(
    layers, total, x_ref, t_ref, up_ref, down_ref, w_ref, u_ref, a_ref, h_ref, gu_ref, gd_ref,
    h_v, y_v, t_v, w_v, u_v, act_v, d_v, a_v, sums, in1, in2, in3,
    w_sem, u_sem, act_sem, h_sem, t_sem, back_u_sem, back_a_sem, back_h_sem, out_sem, free1, *sems,
):
    def load_a(l):
        return pltpu.make_async_copy(a_ref.at[l], a_v, back_a_sem)

    def load_w(i):
        l, s = layers - 1 - lax.div(i, 4), lax.rem(i, 4)
        ws = lax.rem(i, 2)

        @pl.when(s == 0)
        def _():
            pltpu.make_async_copy(up_ref.at[l], w_v.at[ws, 0], w_sem.at[ws, 0]).start()
            pltpu.make_async_copy(down_ref.at[l], w_v.at[ws, 1], w_sem.at[ws, 1]).start()

        @pl.when(s > 0)
        def _():
            c = 3 * l + s - 1
            for k in (0, 1):
                pltpu.make_async_copy(w_ref.at[c, k], w_v.at[ws, k], w_sem.at[ws, k]).start()

    def prefetch():
        load_a(layers - 1).start()
        load_w(0)

    drain = forward_pass(
        layers, total, prefetch, x_ref, t_ref, up_ref, down_ref, w_ref, u_ref, a_ref, h_ref,
        h_v, y_v, t_v, w_v, u_v, act_v, w_sem, u_sem, act_sem, h_sem, t_sem, *sems[:13],
    )
    backward_pass(
        layers, load_a, load_w, x_ref, h_ref, up_ref, u_ref, gu_ref, gd_ref,
        h_v, y_v, w_v, u_v, d_v, a_v, t_v, sums, in1, in2, in3,
        w_sem, back_u_sem, back_h_sem, out_sem, free1, *sems[13:],
    )
    drain()


def any_specs(count):
    return [pl.BlockSpec(memory_space=pl.ANY)] * count


def local_step(hidden, targets, w_up, w_down, total_tokens):
    layers, d, own = w_up.shape
    m = hidden.shape[0]
    tm = m // TILES
    groups = 3 * layers
    dma = pltpu.SemaphoreType.DMA
    out = pl.pallas_call(
        functools.partial(kernel, layers, float(total_tokens)),
        out_shape=[
            jax.ShapeDtypeStruct((groups, 2, d, own), BF16),
            jax.ShapeDtypeStruct((4 * layers, m, own), BF16),
            jax.ShapeDtypeStruct((layers, m, own), BF16),
            jax.ShapeDtypeStruct((layers - 1, m, d), BF16),
            jax.ShapeDtypeStruct((layers, d, own), F32),
            jax.ShapeDtypeStruct((layers, own, d), F32),
        ],
        in_specs=any_specs(4),
        out_specs=any_specs(6),
        scratch_shapes=[
            pltpu.VMEM((m, d), BF16),
            pltpu.VMEM((m, d), F32),
            pltpu.VMEM((m, d), BF16),
            pltpu.VMEM((2, 2, d, own), BF16),
            pltpu.VMEM((2, tm, own), BF16),
            pltpu.VMEM((2, tm, own), BF16),
            pltpu.VMEM((m, own), BF16),
            pltpu.VMEM((m, own), BF16),
            pltpu.VMEM((3, d, own), F32),
            pltpu.VMEM((2, d // 2, own), F32),
            pltpu.VMEM((2, 2, d // 8, own), F32),
            pltpu.VMEM((2, 2, d // 16, own), F32),
            dma((2, 2)), dma((2,)), dma((2,)), dma((TILES,)), dma((2,)),
            dma((2,)), dma, dma, dma((2, 2)), pltpu.SemaphoreType.REGULAR,
        ] + [dma((groups,))] * 13 + [dma((2 * layers,))] * 2 + [dma((2, 2 * layers))] * 8 + [dma((2 * layers,))] * 2,
        compiler_params=pltpu.CompilerParams(collective_id=0, has_side_effects=True, vmem_limit_bytes=66_900_000),
        name="gradients",
    )(hidden, targets, w_up, w_down)
    return out[4], out[5]


def solution(mesh):
    def grad_step(hidden_in, targets, w_up, w_down):
        step_fn = functools.partial(local_step, total_tokens=hidden_in.shape[0])
        mapped = jax.shard_map(step_fn, mesh=mesh, in_specs=(P("dp", None), P("dp", None), P(None, None, "tp"), P(None, "tp", None)), out_specs=(P(None, None, "tp"), P(None, "tp", None)), check_vma=False)
        return mapped(hidden_in, targets, w_up, w_down)

    return grad_step
```

```python
import functools
import math
import jax
import jax.numpy as jnp
from jax import lax
from jax.experimental import pallas as pl
from jax.experimental.pallas import tpu as pltpu
from jax.sharding import PartitionSpec as P

BF16 = jnp.bfloat16
F32 = jnp.float32
MESH = pl.DeviceIdType.MESH
TILES = 2
PARTS_FORWARD = 8
PARTS_BACKWARD = 4
K0 = math.sqrt(2.0 / math.pi)
K1 = 0.044715 * K0
BY_ROWS = (((0,), (0,)), ((), ()))
BY_COLS = (((1,), (1,)), ((), ()))


def dot_cols(lhs, rhs):
    return lax.dot_general(lhs, rhs, BY_COLS, preferred_element_type=F32)


def dot_rows(lhs, rhs):
    return lax.dot_general(lhs, rhs, BY_ROWS, preferred_element_type=F32)


class Place:
    def __init__(self):
        z = lax.axis_index("tp")
        d = lax.axis_index("dp")
        self.core = lax.rem(d, 2)
        self.x = lax.rem(lax.div(d, 2), 2)
        self.y = lax.div(d, 4)
        self.inner = (z == 1) | (z == 2)
        self.near = {"tp": z + 1 - 2 * lax.rem(z, 2)}
        self.middle = {"tp": 3 - z}
        self.x_dev = {"dp": self.index(self.y, 1 - self.x, self.core)}
        self.y_dev = {"dp": self.index(1 - self.y, self.x, self.core)}
        self.partner = {"dp": self.index(self.y, self.x, 1 - self.core)}

    @staticmethod
    def index(y, x, core):
        return y * 4 + x * 2 + core


def remote(src, dst, send_sem, recv_sem, device):
    return pltpu.make_async_remote_copy(src_ref=src, dst_ref=dst, send_sem=send_sem, recv_sem=recv_sem, device_id=device, device_id_type=MESH)


def meet(devices):
    barrier = pltpu.get_barrier_semaphore()
    for device in devices:
        pl.semaphore_signal(barrier, inc=1, device_id=device, device_id_type=MESH)
    pl.semaphore_wait(barrier, len(devices))


FORWARD_TIMES = {
    "F": (0, 0, 0, 1, 1, 5, 14, 16, 22, 11, 12, 23),
    "Z": (1, 6, 1),
    "1": (0, 0, 1, 3, 6, 13, 18, 21, 27, 36, 41, 47),
    "2": (1, 1, 4, 7, 16, 18, 25, 32, 34, 44, 46, 54),
    "3": (3, 5, 9, 14, 19, 24, 32, 36, 39, 48, 51, 57),
    "L": (3, 6, 10, 12, 19, 23, 26, 29, 34, 38, 42, 46, 50, 54, 59),
}

BACKWARD_TIMES = (
    (0, 6, 32, 38, 64, 70, 96, 102),
    (2, 8, 33, 40, 65, 71, 97, 128),
    (7, 14, 39, 46, 74, 76, 133, 134),
    (10, 19, 45, 51, 77, 79, 135, 137),
    (15, 35, 48, 66, 81, 84, 143, 144),
    (50, 42, 81, 80, 131, 131, 147, 151),
    (99, 96, 145, 151, 145, 145, 151, 151),
)


def forward_plan():
    events = []
    for rank, (kind, times) in enumerate(FORWARD_TIMES.items()):
        for i, n in enumerate(times):
            c = i + 1 if kind in "ZL" else i
            age = 3 * c - 2.5 if kind == "Z" else c if kind != "L" else 3 * (c // 4) + (c % 4 - 1 if c % 4 else -0.5)
            events.append((n, age, rank, kind, c))
    return [(n, kind, c) for n, _, _, kind, c in sorted(events)]


def backward_plan():
    return [(p, k, j) for p, j, k in sorted((p, j, k + 1) for k, times in enumerate(BACKWARD_TIMES) for j, p in enumerate(times))]


def at_step(plan, now, block, steps, run):
    for b in sorted({e[0] // block for e in plan}):
        here = [e for e in plan if e[0] // block == b and e[0] % block in steps]
        if not here:
            continue

        @pl.when(lax.div(now, block) == b)
        def _():
            for n in sorted({e[0] for e in here}):
                @pl.when(now == n)
                def _():
                    for e in here:
                        if e[0] == n:
                            run(e[1], e[2])


def forward_pass(
    layers, total, prefetch, x_ref, t_ref, up_ref, down_ref, w_ref, u_ref, a_ref, h_ref,
    h_v, y_v, t_v, w_v, u_v, a_v, w_sem, u_sem, a_sem, h_sem, t_sem,
    zs, zr, fs, xs, xr, ys, yr, as_, ar, bs, br, ds, dr,
):
    plan = forward_plan()
    me = Place()
    groups = 3 * layers
    m, d = h_v.shape
    tm = m // TILES
    part = d // 8
    half = part // 2
    last_n = 4 * TILES * layers - 1
    wide = min(256, d)

    def rows(y, x):
        return pl.multiple_of(me.core * (4 * part) + (y * 2 + x) * part, part)

    mine, of_x, of_y, of_d = rows(me.y, me.x), rows(me.y, 1 - me.x), rows(1 - me.y, me.x), rows(1 - me.y, 1 - me.x)
    half_mine = pl.multiple_of(me.core * (4 * part), 4 * part)
    half_other = pl.multiple_of((1 - me.core) * (4 * part), 4 * part)

    def piece(c, start, size):
        return w_ref.at[c, :, pl.ds(start, size), :]

    def z_copy(c):
        return remote(piece(c, mine, part), piece(c, mine, part), zs.at[c], zr.at[c], me.near)

    def f_copy(c):
        to, device = (c + 2, me.middle) if c % 3 == 0 else (c, me.near)
        return remote(piece(c, mine, part), piece(to, mine, part), fs.at[c], zr.at[to], device)

    def x_copy(c, start):
        return remote(piece(c, start, part), piece(c, start, part), xs.at[c], xr.at[c], me.x_dev)

    def y_copy(c, start):
        return remote(piece(c, start, part), piece(c, start, part), ys.at[c], yr.at[c], me.y_dev)

    def a_copy(c, start):
        return remote(piece(c, start, half), piece(c, start, half), as_.at[c], ar.at[c], me.y_dev)

    def b_copy(c, start):
        return remote(piece(c, start + half, half), piece(c, start + half, half), bs.at[c], br.at[c], me.x_dev)

    def d_copy(c, start):
        return remote(piece(c, start, 4 * part), piece(c, start, 4 * part), ds.at[c], dr.at[c], me.partner)

    def send_own(l, c, device):
        for k, own in enumerate((up_ref, down_ref)):
            remote(own.at[l, pl.ds(mine, part), :], w_ref.at[c, k, pl.ds(mine, part), :], zs.at[c], zr.at[c], device).start()

    def load_w(g):
        l, s, ws = g // 4, g % 4, g % 2
        c = 3 * l + s - 1
        if s > 0:
            d_copy(c, half_other).wait_recv()
        for k, own in enumerate((up_ref, down_ref)):
            pltpu.make_async_copy(own.at[l] if s == 0 else w_ref.at[c, k], w_v.at[ws, k], w_sem.at[ws, k]).start()

    def run(kind, c):
        if kind == "Z":
            send_own(c, 3 * c, me.near)

            @pl.when(me.inner)
            def _():
                send_own(c, 3 * c + 1, me.middle)
        elif kind == "F":
            @pl.when(me.inner)
            def _():
                z_copy(c).wait_recv()
                f_copy(c).start()
        elif kind == "1":
            @pl.when(jnp.logical_not(me.inner))
            def _():
                z_copy(c).wait_recv()

            x_copy(c, mine).start()
            y_copy(c, mine).start()
        elif kind == "2":
            x_copy(c, of_x).wait_recv()
            a_copy(c, of_x).start()
            y_copy(c, of_y).wait_recv()
            b_copy(c, of_y).start()
        elif kind == "3":
            a_copy(c, of_d).wait_recv()
            b_copy(c, of_d).wait_recv()
            d_copy(c, half_mine).start()
        else:
            load_w(c)

    first = pltpu.make_async_copy(x_ref, h_v, t_sem.at[0])
    first.start()
    load_w(0)
    meet([me.near, me.middle, me.x_dev, me.y_dev, me.partner])
    run("Z", 0)
    last = pltpu.make_async_copy(t_ref, t_v, t_sem.at[1])
    last.start()
    y_v[...] = jnp.zeros_like(y_v)
    first.wait()

    def tile_of(n):
        return lax.rem(n, TILES)

    def there(n):
        return pl.ds(pl.multiple_of(tile_of(n) * tm, tm), tm)

    def slot_of(n):
        return lax.rem(lax.div(n, TILES), 2)

    def wait_w(n):
        for k in (0, 1):
            pltpu.make_async_copy(up_ref.at[0], w_v.at[slot_of(n), k], w_sem.at[slot_of(n), k]).wait()

    def u_copy(n):
        slot = lax.rem(n, 2)
        return pltpu.make_async_copy(u_v.at[slot], u_ref.at[lax.div(n, TILES), there(n), :], u_sem.at[slot])

    def a_out(n):
        slot = lax.rem(n, 2)
        return pltpu.make_async_copy(a_v.at[slot], a_ref.at[lax.div(n, 4 * TILES), there(n), :], a_sem.at[slot])

    def h_out(dst, n):
        return pltpu.make_async_copy(h_v.at[there(n), :], dst.at[there(n), :], h_sem.at[tile_of(n)])

    def is_block(n, s):
        return lax.rem(lax.div(n, TILES), 4) == s

    def settle_rows(n):
        l = lax.div(n, 4 * TILES)

        @pl.when(l > 0)
        def _():
            h_out(h_ref.at[0], n).wait()

        def sweep(last_layer):
            size = min(32, tm)

            def body(i, carry):
                few = pl.ds(pl.multiple_of(tile_of(n) * tm + i * size, size), size)
                h_new = (h_v[few, :].astype(F32) + y_v[few, :].astype(BF16).astype(F32)).astype(BF16)
                if last_layer:
                    h_new = ((h_new.astype(F32) - t_v[few, :].astype(F32)) / total).astype(BF16)
                h_v[few, :] = h_new
                y_v[few, :] = h_new.astype(F32) if last_layer else jnp.zeros((size, d), F32)
                return carry

            lax.fori_loop(0, tm // size, body, 0)

        @pl.when(l < layers - 1)
        def _():
            sweep(False)
            h_out(h_ref.at[l], n).start()

        @pl.when(l == layers - 1)
        def _():
            sweep(True)

    def step(n, carry):
        here, slot, ws = there(n), lax.rem(n, 2), slot_of(n)

        @pl.when(n >= 2)
        def _():
            u_copy(n).wait()

        @pl.when((n >= 2) & is_block(n - 2, 0))
        def _():
            a_out(n).wait()

        @pl.when(tile_of(n) == 0)
        def _():
            wait_w(n)

        few = tm // PARTS_FORWARD
        for r in range(0, tm, few):
            some = pl.ds(pl.multiple_of(tile_of(n) * tm + r, few), few)
            for j in range(0, d, wide):
                u = jnp.dot(h_v[some, :], w_v[ws, 0, :, j:j + wide], preferred_element_type=F32).astype(BF16)
                u_v[slot, r:r + few, j:j + wide] = u
                v = u.astype(F32)
                th = jnp.tanh(v * (K0 + K1 * (v * v)))
                hv = 0.5 * v
                a_v[slot, r:r + few, j:j + wide] = (hv + hv * th).astype(BF16)
        u_copy(n).start()

        @pl.when(is_block(n, 0))
        def _():
            a_out(n).start()

        @pl.when(n == last_n - TILES + 1)
        def _():
            prefetch()

        at_step(plan, 2 * n, 8 * TILES, range(0, 8 * TILES, 2), run)
        for j in range(0, d, wide):
            y_v[here, j:j + wide] += jnp.dot(a_v[slot], w_v[ws, 1, :, j:j + wide], preferred_element_type=F32)

        @pl.when(is_block(n, 3))
        def _():
            settle_rows(n)

        at_step(plan, 2 * n + 1, 8 * TILES, range(1, 8 * TILES, 2), run)

        return carry

    last.wait()
    lax.fori_loop(0, last_n + 1, step, 0)
    u_copy(last_n - 1).wait()
    u_copy(last_n).wait()

    def drain():
        for c in range(groups):
            if c % 3 == 0:
                z_copy(c).wait_send()

            @pl.when(me.inner)
            def _():
                f_copy(c).wait_send()
                if c % 3 == 1:
                    z_copy(c).wait_send()

            x_copy(c, mine).wait_send()
            y_copy(c, mine).wait_send()
            a_copy(c, of_x).wait_send()
            b_copy(c, of_y).wait_send()
            d_copy(c, half_mine).wait_send()

    return drain


def backward_pass(
    layers, load_a, load_w, x_ref, h_ref, up_ref, u_ref, gu_ref, gd_ref,
    g_v, acc_v, w_v, u_v, d_v, a_v, h_v, sums, in1, in2, in3,
    w_sem, u_sem, h_sem, out_sem, free1,
    s1, r1, s2, r2, s3, r3, s4, r4, s5, r5, s6, r6,
):
    plan = backward_plan()
    me = Place()
    m, d = g_v.shape
    tm = m // TILES
    hd, qd = d // 2, d // 4
    e8, e16 = d // 8, d // 16
    wide = min(256, d)
    broad = d // 2

    def at(value, size):
        return pl.ds(pl.multiple_of(value, size), size)

    own = me.core * hd
    own_rows, other_rows = at(own, hd), at(hd - own, hd)
    a_base, b_base = own, own + qd
    a_keep, a_give = at(a_base + me.x * e8, e8), at(a_base + (1 - me.x) * e8, e8)
    b_keep, b_give = at(b_base + me.y * e8, e8), at(b_base + (1 - me.y) * e8, e8)
    a_last, a_pass = at(a_base + me.x * e8 + me.y * e16, e16), at(a_base + me.x * e8 + (1 - me.y) * e16, e16)
    b_last, b_pass = at(b_base + me.y * e8 + me.x * e16, e16), at(b_base + me.y * e8 + (1 - me.x) * e16, e16)

    def room(j):
        return lax.rem(j, 2) * (1 + lax.rem(lax.div(j, 2), 2))

    def c1(j):
        return remote(sums.at[room(j), other_rows, :], in1.at[lax.rem(j, 2)], s1.at[j], r1.at[j], me.partner)

    def c2(j):
        q, r = room(j), lax.rem(j, 2)
        return (remote(sums.at[q, a_give, :], in2.at[r, 0], s2.at[0, j], r2.at[0, j], me.x_dev),
                remote(sums.at[q, b_give, :], in2.at[r, 1], s2.at[1, j], r2.at[1, j], me.y_dev))

    def c3(j):
        q, r = room(j), lax.rem(j, 2)
        return (remote(sums.at[q, a_pass, :], in3.at[r, 0], s3.at[0, j], r3.at[0, j], me.y_dev),
                remote(sums.at[q, b_pass, :], in3.at[r, 1], s3.at[1, j], r3.at[1, j], me.x_dev))

    def c4(j, ref, a_rows, b_rows):
        q, dst = room(j), ref.at[layers - 1 - lax.div(j, 2)]
        return (remote(sums.at[q, a_rows, :], dst.at[a_rows, :], s4.at[0, j], r4.at[0, j], me.y_dev),
                remote(sums.at[q, b_rows, :], dst.at[b_rows, :], s4.at[1, j], r4.at[1, j], me.x_dev))

    def keep(j, ref):
        q, dst = room(j), ref.at[layers - 1 - lax.div(j, 2)]
        return (pltpu.make_async_copy(sums.at[q, a_last, :], dst.at[a_last, :], out_sem.at[0, lax.rem(j, 2)]),
                pltpu.make_async_copy(sums.at[q, b_last, :], dst.at[b_last, :], out_sem.at[1, lax.rem(j, 2)]))

    def c5(j, ref, a_rows, b_rows):
        dst = ref.at[layers - 1 - lax.div(j, 2)]
        return (remote(dst.at[a_rows, :], dst.at[a_rows, :], s5.at[0, j], r5.at[0, j], me.x_dev),
                remote(dst.at[b_rows, :], dst.at[b_rows, :], s5.at[1, j], r5.at[1, j], me.y_dev))

    def c6(j, ref, which):
        dst = ref.at[layers - 1 - lax.div(j, 2)]
        return remote(dst.at[which, :], dst.at[which, :], s6.at[j], r6.at[j], me.partner)

    def add(j, start, size, buffer):
        q = room(j)
        step = min(32, size)

        def body(i, carry):
            there = pl.ds(pl.multiple_of(start + i * step, step), step)
            sums[q, there, :] = sums[q, there, :] + buffer[pl.ds(pl.multiple_of(i * step, step), step), :]
            return carry

        lax.fori_loop(0, size // step, body, 0)

    def step1(j):
        @pl.when(j >= 2)
        def _():
            pl.semaphore_wait(free1, 1)

        c1(j).start()

    def step2(j):
        c1(j).wait_recv()
        add(j, own, hd, in1.at[lax.rem(j, 2)])

        @pl.when(j < 2 * layers - 2)
        def _():
            pl.semaphore_signal(free1, inc=1, device_id=me.partner, device_id_type=MESH)

        for copy in c2(j):
            copy.start()

    def step3(j):
        r, got, put = lax.rem(j, 2), c2(j), c3(j)
        for k, start in enumerate((a_base + me.x * e8, b_base + me.y * e8)):
            got[k].wait_recv()
            add(j, start, e8, in2.at[r, k])
            put[k].start()

    def step4(j, ref):
        r, got, put, local = lax.rem(j, 2), c3(j), c4(j, ref, a_last, b_last), keep(j, ref)
        for k, start in enumerate((a_base + me.x * e8 + me.y * e16, b_base + me.y * e8 + me.x * e16)):
            got[k].wait_recv()
            add(j, start, e16, in3.at[r, k])
            put[k].start()
            local[k].start()

    def step5(j, ref):
        got, put, local = c4(j, ref, a_pass, b_pass), c5(j, ref, a_keep, b_keep), keep(j, ref)
        for k in (0, 1):
            local[k].wait()
            got[k].wait_recv()
            put[k].start()

    def step6(j, ref):
        for copy in c5(j, ref, a_give, b_give):
            copy.wait_recv()
        c6(j, ref, own_rows).start()

    def step7(j, ref):
        c6(j, ref, other_rows).wait_recv()

    def settle(j, ref):
        c1(j).wait_send()
        for copy in c2(j) + c3(j) + c4(j, ref, a_last, b_last):
            copy.wait_send()

    def finish(j, ref):
        for copy in c5(j, ref, a_keep, b_keep):
            copy.wait_send()
        c6(j, ref, own_rows).wait_send()

    def run(k, j):
        ref = gd_ref if j % 2 == 0 else gu_ref
        (step1, step2, step3, step4, step5, step6, step7)[k - 1](*((j,) if k <= 3 else (j, ref)))

    def at_place(tau, p, steps):
        at_step(plan, 32 * tau + p, 32, steps, run)

    def u_copy(n):
        l, s, t, slot = layers - 1 - lax.div(n, 4 * TILES), lax.rem(lax.div(n, TILES), 4), lax.rem(n, TILES), lax.rem(n, 2)
        return pltpu.make_async_copy(u_ref.at[4 * l + s, pl.ds(t * tm, tm), :], u_v.at[slot], u_sem.at[slot])

    def load_h(l):
        @pl.when(l == 0)
        def _():
            pltpu.make_async_copy(x_ref, h_v, h_sem).start()

        @pl.when(l > 0)
        def _():
            pltpu.make_async_copy(h_ref.at[l - 1], h_v, h_sem).start()

    def wait_w(i):
        for k in (0, 1):
            pltpu.make_async_copy(up_ref.at[0], w_v.at[lax.rem(i, 2), k], w_sem.at[lax.rem(i, 2), k]).wait()

    def next_g():
        step = min(64, m)

        def body(i, carry):
            here = pl.ds(pl.multiple_of(i * step, step), step)
            g_v[here, :] = acc_v[here, :].astype(BF16)
            acc_v[here, :] = g_v[here, :].astype(F32)
            return carry

        lax.fori_loop(0, m // step, body, 0)

    load_h(layers - 1)
    u_copy(0).start()
    tiles_total = TILES * (4 * (layers - 1) + 1)
    groups = 4 * (layers - 1) + 1

    def layer(tau, carry):
        l = layers - 1 - tau
        down, up = 2 * tau, 2 * tau + 1
        room_down, room_up = room(down), room(up)
        load_a(l).wait()

        @pl.when(tau > 0)
        def _():
            settle(down - 2, gd_ref)

        def product(room_j, lhs, rhs, base):
            def body(i, carry):
                cols = at(lax.rem(i + 1 + me.core, 2) * broad, broad)
                sums[room_j, cols, :] = dot_rows(lhs[:, cols], rhs[...])
                at_place(tau, base + i, (base, base + 1))
                return carry

            lax.fori_loop(0, 2, body, 0)

        product(room_down, a_v, g_v, 0)

        @pl.when(l > 0)
        def _():
            load_a(l - 1).start()

        def step(n, carry):
            k = 4 * TILES * tau + n
            block, slot = 4 * tau + lax.div(n, TILES), lax.rem(k, 2)
            ws = lax.rem(block, 2)
            here = pl.ds(pl.multiple_of(lax.rem(n, TILES) * tm, tm), tm)

            @pl.when(k + 1 < tiles_total)
            def _():
                u_copy(k + 1).start()

            @pl.when(lax.rem(n, TILES) == 0)
            def _():
                @pl.when(block + 1 < groups)
                def _():
                    load_w(block + 1)

                wait_w(block)

            u_copy(k).wait()
            few = tm // PARTS_BACKWARD
            for r in range(0, tm, few):
                some = pl.ds(pl.multiple_of(lax.rem(n, TILES) * tm + r, few), few)
                for j in range(0, d, wide):
                    da = dot_cols(g_v[some, :], w_v[ws, 1, j:j + wide, :])
                    v = u_v[slot, r:r + few, j:j + wide].astype(F32)
                    v2 = v * v
                    th = jnp.tanh(v * (K0 + K1 * v2))
                    slope = (1.0 + th) * (0.5 + (v * (1.0 - th)) * ((0.5 * K0) + (1.5 * K1) * v2))
                    d_v[some, j:j + wide] = (da * slope).astype(BF16)
            place = 2 * n + jnp.where(n >= TILES, 4, 2)
            at_place(tau, place, [2, 4] + list(range(8, 20, 2)))

            @pl.when(l > 0)
            def _():
                for j in range(0, d, wide):
                    acc_v[here, j:j + wide] += dot_cols(d_v[here, :], w_v[ws, 0, j:j + wide, :])

            at_place(tau, place + 1, [3, 5] + list(range(9, 20, 2)))

            @pl.when(n == TILES - 1)
            def _():
                pltpu.make_async_copy(x_ref, h_v, h_sem).wait()

                @pl.when(tau >= 2)
                def _():
                    settle(up - 4, gu_ref)

                product(room_up, h_v, d_v, 6)

                @pl.when(l > 0)
                def _():
                    load_h(l - 1)

            return carry

        lax.fori_loop(0, jnp.where(l > 0, 4 * TILES, TILES), step, 0)

        @pl.when(l > 0)
        def _():
            next_g()
            at_place(tau, 20, (20,))

        return carry

    lax.fori_loop(0, layers, layer, 0)
    for p, k, j in plan:
        if p >= 32 * layers:
            run(k, j)
    for j in range(2 * layers):
        ref = gd_ref if j % 2 == 0 else gu_ref
        finish(j, ref)
        if j >= 2 * layers - 3 and j != 2 * layers - 4:
            settle(j, ref)


def kernel(
    layers, total, x_ref, t_ref, up_ref, down_ref, w_ref, u_ref, a_ref, h_ref, gu_ref, gd_ref,
    h_v, y_v, t_v, w_v, u_v, act_v, d_v, a_v, sums, in1, in2, in3,
    w_sem, u_sem, act_sem, h_sem, t_sem, back_u_sem, back_a_sem, back_h_sem, out_sem, free1, *sems,
):
    def load_a(l):
        return pltpu.make_async_copy(a_ref.at[l], a_v, back_a_sem)

    def load_w(i):
        l, s = layers - 1 - lax.div(i, 4), lax.rem(i, 4)
        ws = lax.rem(i, 2)

        @pl.when(s == 0)
        def _():
            pltpu.make_async_copy(up_ref.at[l], w_v.at[ws, 0], w_sem.at[ws, 0]).start()
            pltpu.make_async_copy(down_ref.at[l], w_v.at[ws, 1], w_sem.at[ws, 1]).start()

        @pl.when(s > 0)
        def _():
            c = 3 * l + s - 1
            for k in (0, 1):
                pltpu.make_async_copy(w_ref.at[c, k], w_v.at[ws, k], w_sem.at[ws, k]).start()

    def prefetch():
        load_a(layers - 1).start()
        load_w(0)

    drain = forward_pass(
        layers, total, prefetch, x_ref, t_ref, up_ref, down_ref, w_ref, u_ref, a_ref, h_ref,
        h_v, y_v, t_v, w_v, u_v, act_v, w_sem, u_sem, act_sem, h_sem, t_sem, *sems[:13],
    )
    backward_pass(
        layers, load_a, load_w, x_ref, h_ref, up_ref, u_ref, gu_ref, gd_ref,
        h_v, y_v, w_v, u_v, d_v, a_v, t_v, sums, in1, in2, in3,
        w_sem, back_u_sem, back_h_sem, out_sem, free1, *sems[13:],
    )
    drain()


def any_specs(count):
    return [pl.BlockSpec(memory_space=pl.ANY)] * count


def local_step(hidden, targets, w_up, w_down, total_tokens):
    layers, d, own = w_up.shape
    m = hidden.shape[0]
    tm = m // TILES
    groups = 3 * layers
    dma = pltpu.SemaphoreType.DMA
    out = pl.pallas_call(
        functools.partial(kernel, layers, float(total_tokens)),
        out_shape=[
            jax.ShapeDtypeStruct((groups, 2, d, own), BF16),
            jax.ShapeDtypeStruct((4 * layers, m, own), BF16),
            jax.ShapeDtypeStruct((layers, m, own), BF16),
            jax.ShapeDtypeStruct((layers - 1, m, d), BF16),
            jax.ShapeDtypeStruct((layers, d, own), F32),
            jax.ShapeDtypeStruct((layers, own, d), F32),
        ],
        in_specs=any_specs(4),
        out_specs=any_specs(6),
        scratch_shapes=[
            pltpu.VMEM((m, d), BF16),
            pltpu.VMEM((m, d), F32),
            pltpu.VMEM((m, d), BF16),
            pltpu.VMEM((2, 2, d, own), BF16),
            pltpu.VMEM((2, tm, own), BF16),
            pltpu.VMEM((2, tm, own), BF16),
            pltpu.VMEM((m, own), BF16),
            pltpu.VMEM((m, own), BF16),
            pltpu.VMEM((3, d, own), F32),
            pltpu.VMEM((2, d // 2, own), F32),
            pltpu.VMEM((2, 2, d // 8, own), F32),
            pltpu.VMEM((2, 2, d // 16, own), F32),
            dma((2, 2)), dma((2,)), dma((2,)), dma((TILES,)), dma((2,)),
            dma((2,)), dma, dma, dma((2, 2)), pltpu.SemaphoreType.REGULAR,
        ] + [dma((groups,))] * 13 + [dma((2 * layers,))] * 2 + [dma((2, 2 * layers))] * 8 + [dma((2 * layers,))] * 2,
        compiler_params=pltpu.CompilerParams(collective_id=0, has_side_effects=True, vmem_limit_bytes=66_900_000),
        name="gradients",
    )(hidden, targets, w_up, w_down)
    return out[4], out[5]


def solution(mesh):
    def grad_step(hidden_in, targets, w_up, w_down):
        step_fn = functools.partial(local_step, total_tokens=hidden_in.shape[0])
        mapped = jax.shard_map(step_fn, mesh=mesh, in_specs=(P("dp", None), P("dp", None), P(None, None, "tp"), P(None, "tp", None)), out_specs=(P(None, None, "tp"), P(None, "tp", None)), check_vma=False)
        return mapped(hidden_in, targets, w_up, w_down)

    return grad_step
```

```python
import functools
import math
import jax
import jax.numpy as jnp
from jax import lax
from jax.experimental import pallas as pl
from jax.experimental.pallas import tpu as pltpu
from jax.sharding import PartitionSpec as P

BF16 = jnp.bfloat16
F32 = jnp.float32
MESH = pl.DeviceIdType.MESH
TILES = 2
PARTS_FORWARD = 8
PARTS_BACKWARD = 4
K0 = math.sqrt(2.0 / math.pi)
K1 = 0.044715 * K0
BY_ROWS = (((0,), (0,)), ((), ()))
BY_COLS = (((1,), (1,)), ((), ()))


def dot_cols(lhs, rhs):
    return lax.dot_general(lhs, rhs, BY_COLS, preferred_element_type=F32)


def dot_rows(lhs, rhs):
    return lax.dot_general(lhs, rhs, BY_ROWS, preferred_element_type=F32)


class Place:
    def __init__(self):
        z = lax.axis_index("tp")
        d = lax.axis_index("dp")
        self.core = lax.rem(d, 2)
        self.x = lax.rem(lax.div(d, 2), 2)
        self.y = lax.div(d, 4)
        self.inner = (z == 1) | (z == 2)
        self.near = {"tp": z + 1 - 2 * lax.rem(z, 2)}
        self.middle = {"tp": 3 - z}
        self.x_dev = {"dp": self.index(self.y, 1 - self.x, self.core)}
        self.y_dev = {"dp": self.index(1 - self.y, self.x, self.core)}
        self.partner = {"dp": self.index(self.y, self.x, 1 - self.core)}

    @staticmethod
    def index(y, x, core):
        return y * 4 + x * 2 + core


def remote(src, dst, send_sem, recv_sem, device):
    return pltpu.make_async_remote_copy(src_ref=src, dst_ref=dst, send_sem=send_sem, recv_sem=recv_sem, device_id=device, device_id_type=MESH)


def meet(devices):
    barrier = pltpu.get_barrier_semaphore()
    for device in devices:
        pl.semaphore_signal(barrier, inc=1, device_id=device, device_id_type=MESH)
    pl.semaphore_wait(barrier, len(devices))


FORWARD_TIMES = {
    "F": (0, 0, 0, 1, 2, 5, 14, 13, 24, 25, 25, 33),
    "Z": (1, 6, 14),
    "1": (0, 0, 1, 4, 7, 14, 20, 21, 30, 35, 38, 45),
    "2": (1, 2, 4, 11, 17, 19, 28, 31, 35, 43, 48, 51),
    "3": (2, 5, 7, 15, 20, 22, 32, 36, 38, 46, 51, 55),
    "L": (3, 6, 9, 12, 17, 22, 25, 27, 34, 38, 42, 43, 49, 54, 58),
}

BACKWARD_TIMES = (
    (0, 6, 32, 38, 64, 70, 96, 102),
    (2, 8, 34, 40, 66, 71, 98, 103),
    (7, 13, 41, 44, 74, 75, 128, 128),
    (11, 17, 46, 47, 77, 79, 131, 132),
    (15, 33, 49, 51, 80, 82, 133, 134),
    (83, 76, 148, 81, 103, 133, 137, 148),
    (99, 103, 151, 135, 143, 138, 151, 149),
)


def forward_plan():
    events = []
    for rank, (kind, times) in enumerate(FORWARD_TIMES.items()):
        for i, n in enumerate(times):
            c = i + 1 if kind in "ZL" else i
            age = 3 * c - 2.5 if kind == "Z" else c if kind != "L" else 3 * (c // 4) + (c % 4 - 1 if c % 4 else -0.5)
            events.append((n, age, rank, kind, c))
    return [(n, kind, c) for n, _, _, kind, c in sorted(events)]


def backward_plan():
    return [(p, k, j) for p, j, k in sorted((p, j, k + 1) for k, times in enumerate(BACKWARD_TIMES) for j, p in enumerate(times))]


def at_step(plan, now, block, steps, run):
    for b in sorted({e[0] // block for e in plan}):
        here = [e for e in plan if e[0] // block == b and e[0] % block in steps]
        if not here:
            continue

        @pl.when(lax.div(now, block) == b)
        def _():
            for n in sorted({e[0] for e in here}):
                @pl.when(now == n)
                def _():
                    for e in here:
                        if e[0] == n:
                            run(e[1], e[2])


def forward_pass(
    layers, total, prefetch, x_ref, t_ref, up_ref, down_ref, w_ref, u_ref, a_ref, h_ref,
    h_v, y_v, t_v, w_v, u_v, a_v, w_sem, u_sem, a_sem, h_sem, t_sem,
    zs, zr, fs, ms, mr, mf, xs, xr, ys, yr, as_, ar, bs, br, ds, dr,
):
    plan = forward_plan()
    me = Place()
    groups = 3 * layers
    m, d = h_v.shape
    tm = m // TILES
    part = d // 8
    half = part // 2
    last_n = 4 * TILES * layers - 1
    wide = min(256, d)

    def rows(y, x):
        return pl.multiple_of(me.core * (4 * part) + (y * 2 + x) * part, part)

    mine, of_x, of_y, of_d = rows(me.y, me.x), rows(me.y, 1 - me.x), rows(1 - me.y, me.x), rows(1 - me.y, 1 - me.x)
    half_mine = pl.multiple_of(me.core * (4 * part), 4 * part)
    half_other = pl.multiple_of((1 - me.core) * (4 * part), 4 * part)

    def piece(c, start, size):
        return w_ref.at[c, :, pl.ds(start, size), :]

    def more(c):
        return d // 64 if c >= 3 else 0

    def z_rows(c):
        return [(mine, part, zs, zr, fs)] + ([(of_d + half - more(c), 2 * more(c), ms, mr, mf)] if more(c) else [])

    def z_copies(c):
        return [remote(piece(c, start, size), piece(c, start, size), send.at[c], recv.at[c], me.near) for start, size, send, recv, _ in z_rows(c)]

    def f_copies(c):
        to, device = (c + 2, me.middle) if c % 3 == 0 else (c, me.near)
        return [remote(piece(c, start, size), piece(to, start, size), send.at[c], recv.at[to], device) for start, size, _, recv, send in z_rows(c)]

    def x_copy(c, start):
        return remote(piece(c, start, part), piece(c, start, part), xs.at[c], xr.at[c], me.x_dev)

    def y_copy(c, start):
        return remote(piece(c, start, part), piece(c, start, part), ys.at[c], yr.at[c], me.y_dev)

    def a_copy(c, start):
        size = half - more(c)
        return remote(piece(c, start, size), piece(c, start, size), as_.at[c], ar.at[c], me.y_dev)

    def b_copy(c, start):
        start, size = start + half + more(c), half - more(c)
        return remote(piece(c, start, size), piece(c, start, size), bs.at[c], br.at[c], me.x_dev)

    def d_copy(c, start):
        return remote(piece(c, start, 4 * part), piece(c, start, 4 * part), ds.at[c], dr.at[c], me.partner)

    def send_own(l, c, device):
        for start, size, send, recv, _ in z_rows(c):
            for k, own in enumerate((up_ref, down_ref)):
                there = w_ref.at[c, k, pl.ds(start, size), :]
                remote(own.at[l, pl.ds(start, size), :], there, send.at[c], recv.at[c], device).start()

    def load_w(g):
        l, s, ws = g // 4, g % 4, g % 2
        c = 3 * l + s - 1
        if s > 0:
            d_copy(c, half_other).wait_recv()
        for k, own in enumerate((up_ref, down_ref)):
            pltpu.make_async_copy(own.at[l] if s == 0 else w_ref.at[c, k], w_v.at[ws, k], w_sem.at[ws, k]).start()

    def run(kind, c):
        if kind == "Z":
            send_own(c, 3 * c, me.near)

            @pl.when(me.inner)
            def _():
                send_own(c, 3 * c + 1, me.middle)
        elif kind == "F":
            @pl.when(me.inner)
            def _():
                for copy in z_copies(c):
                    copy.wait_recv()
                for copy in f_copies(c):
                    copy.start()
        elif kind == "1":
            @pl.when(jnp.logical_not(me.inner))
            def _():
                for copy in z_copies(c):
                    copy.wait_recv()

            x_copy(c, mine).start()
            y_copy(c, mine).start()
        elif kind == "2":
            x_copy(c, of_x).wait_recv()
            a_copy(c, of_x).start()
            y_copy(c, of_y).wait_recv()
            b_copy(c, of_y).start()
        elif kind == "3":
            a_copy(c, of_d).wait_recv()
            b_copy(c, of_d).wait_recv()
            d_copy(c, half_mine).start()
        else:
            load_w(c)

    first = pltpu.make_async_copy(x_ref, h_v, t_sem.at[0])
    first.start()
    load_w(0)
    meet([me.near, me.middle, me.x_dev, me.y_dev, me.partner])
    run("Z", 0)
    last = pltpu.make_async_copy(t_ref, t_v, t_sem.at[1])
    last.start()
    y_v[...] = jnp.zeros_like(y_v)
    first.wait()

    def tile_of(n):
        return lax.rem(n, TILES)

    def there(n):
        return pl.ds(pl.multiple_of(tile_of(n) * tm, tm), tm)

    def slot_of(n):
        return lax.rem(lax.div(n, TILES), 2)

    def wait_w(n):
        for k in (0, 1):
            pltpu.make_async_copy(up_ref.at[0], w_v.at[slot_of(n), k], w_sem.at[slot_of(n), k]).wait()

    def u_copy(n):
        slot = lax.rem(n, 2)
        return pltpu.make_async_copy(u_v.at[slot], u_ref.at[lax.div(n, TILES), there(n), :], u_sem.at[slot])

    def a_out(n):
        slot = lax.rem(n, 2)
        return pltpu.make_async_copy(a_v.at[slot], a_ref.at[lax.div(n, 4 * TILES), there(n), :], a_sem.at[slot])

    def h_out(dst, n):
        return pltpu.make_async_copy(h_v.at[there(n), :], dst.at[there(n), :], h_sem.at[tile_of(n)])

    def is_block(n, s):
        return lax.rem(lax.div(n, TILES), 4) == s

    def settle_rows(n):
        l = lax.div(n, 4 * TILES)

        @pl.when(l > 0)
        def _():
            h_out(h_ref.at[0], n).wait()

        def sweep(last_layer):
            size = min(32, tm)

            def body(i, carry):
                few = pl.ds(pl.multiple_of(tile_of(n) * tm + i * size, size), size)
                h_new = (h_v[few, :].astype(F32) + y_v[few, :].astype(BF16).astype(F32)).astype(BF16)
                if last_layer:
                    h_new = ((h_new.astype(F32) - t_v[few, :].astype(F32)) / total).astype(BF16)
                h_v[few, :] = h_new
                y_v[few, :] = h_new.astype(F32) if last_layer else jnp.zeros((size, d), F32)
                return carry

            lax.fori_loop(0, tm // size, body, 0)

        @pl.when(l < layers - 1)
        def _():
            sweep(False)
            h_out(h_ref.at[l], n).start()

        @pl.when(l == layers - 1)
        def _():
            sweep(True)

    def step(n, carry):
        here, slot, ws = there(n), lax.rem(n, 2), slot_of(n)

        @pl.when(n >= 2)
        def _():
            u_copy(n).wait()

        @pl.when((n >= 2) & is_block(n - 2, 0))
        def _():
            a_out(n).wait()

        @pl.when(tile_of(n) == 0)
        def _():
            wait_w(n)

        few = tm // PARTS_FORWARD
        for r in range(0, tm, few):
            some = pl.ds(pl.multiple_of(tile_of(n) * tm + r, few), few)
            for j in range(0, d, wide):
                u = jnp.dot(h_v[some, :], w_v[ws, 0, :, j:j + wide], preferred_element_type=F32).astype(BF16)
                u_v[slot, r:r + few, j:j + wide] = u
                v = u.astype(F32)
                th = jnp.tanh(v * (K0 + K1 * (v * v)))
                hv = 0.5 * v
                a_v[slot, r:r + few, j:j + wide] = (hv + hv * th).astype(BF16)
        u_copy(n).start()

        @pl.when(is_block(n, 0))
        def _():
            a_out(n).start()

        @pl.when(n == last_n - TILES + 1)
        def _():
            prefetch()

        at_step(plan, 2 * n, 8 * TILES, range(0, 8 * TILES, 2), run)
        for j in range(0, d, wide):
            y_v[here, j:j + wide] += jnp.dot(a_v[slot], w_v[ws, 1, :, j:j + wide], preferred_element_type=F32)

        @pl.when(is_block(n, 3))
        def _():
            settle_rows(n)

        at_step(plan, 2 * n + 1, 8 * TILES, range(1, 8 * TILES, 2), run)

        return carry

    last.wait()
    lax.fori_loop(0, last_n + 1, step, 0)
    u_copy(last_n - 1).wait()
    u_copy(last_n).wait()

    def drain():
        for c in range(groups):
            if c % 3 == 0:
                for copy in z_copies(c):
                    copy.wait_send()

            @pl.when(me.inner)
            def _():
                for copy in f_copies(c) + (z_copies(c) if c % 3 == 1 else []):
                    copy.wait_send()

            x_copy(c, mine).wait_send()
            y_copy(c, mine).wait_send()
            a_copy(c, of_x).wait_send()
            b_copy(c, of_y).wait_send()
            d_copy(c, half_mine).wait_send()

    return drain


def backward_pass(
    layers, load_a, load_w, x_ref, h_ref, up_ref, u_ref, gu_ref, gd_ref,
    g_v, acc_v, w_v, u_v, d_v, a_v, h_v, sums, in1, in2, in3,
    w_sem, u_sem, h_sem, out_sem, free1,
    s1, r1, s2, r2, s3, r3, s4, r4, s5, r5, s6, r6,
):
    plan = backward_plan()
    me = Place()
    m, d = g_v.shape
    tm = m // TILES
    hd, qd = d // 2, d // 4
    e8, e16 = d // 8, d // 16
    wide = min(256, d)
    broad = d // 2

    def at(value, size):
        return pl.ds(pl.multiple_of(value, size), size)

    own = me.core * hd
    own_rows, other_rows = at(own, hd), at(hd - own, hd)
    a_base, b_base = own, own + qd
    a_keep, a_give = at(a_base + me.x * e8, e8), at(a_base + (1 - me.x) * e8, e8)
    b_keep, b_give = at(b_base + me.y * e8, e8), at(b_base + (1 - me.y) * e8, e8)
    a_last, a_pass = at(a_base + me.x * e8 + me.y * e16, e16), at(a_base + me.x * e8 + (1 - me.y) * e16, e16)
    b_last, b_pass = at(b_base + me.y * e8 + me.x * e16, e16), at(b_base + me.y * e8 + (1 - me.x) * e16, e16)

    def room(j):
        return lax.rem(j, 2) * (1 + lax.rem(lax.div(j, 2), 2))

    def c1(j):
        return remote(sums.at[room(j), other_rows, :], in1.at[lax.rem(j, 2)], s1.at[j], r1.at[j], me.partner)

    def c2(j):
        q, r = room(j), lax.rem(j, 2)
        return (remote(sums.at[q, a_give, :], in2.at[r, 0], s2.at[0, j], r2.at[0, j], me.x_dev),
                remote(sums.at[q, b_give, :], in2.at[r, 1], s2.at[1, j], r2.at[1, j], me.y_dev))

    def c3(j):
        q, r = room(j), lax.rem(j, 2)
        return (remote(sums.at[q, a_pass, :], in3.at[r, 0], s3.at[0, j], r3.at[0, j], me.y_dev),
                remote(sums.at[q, b_pass, :], in3.at[r, 1], s3.at[1, j], r3.at[1, j], me.x_dev))

    def c4(j, ref, a_rows, b_rows):
        q, dst = room(j), ref.at[layers - 1 - lax.div(j, 2)]
        return (remote(sums.at[q, a_rows, :], dst.at[a_rows, :], s4.at[0, j], r4.at[0, j], me.y_dev),
                remote(sums.at[q, b_rows, :], dst.at[b_rows, :], s4.at[1, j], r4.at[1, j], me.x_dev))

    def keep(j, ref):
        q, dst = room(j), ref.at[layers - 1 - lax.div(j, 2)]
        return (pltpu.make_async_copy(sums.at[q, a_last, :], dst.at[a_last, :], out_sem.at[0, lax.rem(j, 2)]),
                pltpu.make_async_copy(sums.at[q, b_last, :], dst.at[b_last, :], out_sem.at[1, lax.rem(j, 2)]))

    def c5(j, ref, a_rows, b_rows):
        dst = ref.at[layers - 1 - lax.div(j, 2)]
        return (remote(dst.at[a_rows, :], dst.at[a_rows, :], s5.at[0, j], r5.at[0, j], me.x_dev),
                remote(dst.at[b_rows, :], dst.at[b_rows, :], s5.at[1, j], r5.at[1, j], me.y_dev))

    def c6(j, ref, which):
        dst = ref.at[layers - 1 - lax.div(j, 2)]
        return remote(dst.at[which, :], dst.at[which, :], s6.at[j], r6.at[j], me.partner)

    def add(j, start, size, buffer):
        q = room(j)
        step = min(32, size)

        def body(i, carry):
            there = pl.ds(pl.multiple_of(start + i * step, step), step)
            sums[q, there, :] = sums[q, there, :] + buffer[pl.ds(pl.multiple_of(i * step, step), step), :]
            return carry

        lax.fori_loop(0, size // step, body, 0)

    def step1(j):
        @pl.when(j >= 2)
        def _():
            pl.semaphore_wait(free1, 1)

        c1(j).start()

    def step2(j):
        c1(j).wait_recv()
        add(j, own, hd, in1.at[lax.rem(j, 2)])

        @pl.when(j < 2 * layers - 2)
        def _():
            pl.semaphore_signal(free1, inc=1, device_id=me.partner, device_id_type=MESH)

        for copy in c2(j):
            copy.start()

    def step3(j):
        r, got, put = lax.rem(j, 2), c2(j), c3(j)
        for k, start in enumerate((a_base + me.x * e8, b_base + me.y * e8)):
            got[k].wait_recv()
            add(j, start, e8, in2.at[r, k])
            put[k].start()

    def step4(j, ref):
        r, got, put, local = lax.rem(j, 2), c3(j), c4(j, ref, a_last, b_last), keep(j, ref)
        for k, start in enumerate((a_base + me.x * e8 + me.y * e16, b_base + me.y * e8 + me.x * e16)):
            got[k].wait_recv()
            add(j, start, e16, in3.at[r, k])
            put[k].start()
            local[k].start()

    def step5(j, ref):
        got, put, local = c4(j, ref, a_pass, b_pass), c5(j, ref, a_keep, b_keep), keep(j, ref)
        for k in (0, 1):
            local[k].wait()
            got[k].wait_recv()
            put[k].start()

    def step6(j, ref):
        for copy in c5(j, ref, a_give, b_give):
            copy.wait_recv()
        c6(j, ref, own_rows).start()

    def step7(j, ref):
        c6(j, ref, other_rows).wait_recv()

    def settle(j, ref):
        c1(j).wait_send()
        for copy in c2(j) + c3(j) + c4(j, ref, a_last, b_last):
            copy.wait_send()

    def finish(j, ref):
        for copy in c5(j, ref, a_keep, b_keep):
            copy.wait_send()
        c6(j, ref, own_rows).wait_send()

    def run(k, j):
        ref = gd_ref if j % 2 == 0 else gu_ref
        (step1, step2, step3, step4, step5, step6, step7)[k - 1](*((j,) if k <= 3 else (j, ref)))

    def at_place(tau, p, steps):
        at_step(plan, 32 * tau + p, 32, steps, run)

    def u_copy(n):
        l, s, t, slot = layers - 1 - lax.div(n, 4 * TILES), lax.rem(lax.div(n, TILES), 4), lax.rem(n, TILES), lax.rem(n, 2)
        return pltpu.make_async_copy(u_ref.at[4 * l + s, pl.ds(t * tm, tm), :], u_v.at[slot], u_sem.at[slot])

    def load_h(l):
        @pl.when(l == 0)
        def _():
            pltpu.make_async_copy(x_ref, h_v, h_sem).start()

        @pl.when(l > 0)
        def _():
            pltpu.make_async_copy(h_ref.at[l - 1], h_v, h_sem).start()

    def wait_w(i):
        for k in (0, 1):
            pltpu.make_async_copy(up_ref.at[0], w_v.at[lax.rem(i, 2), k], w_sem.at[lax.rem(i, 2), k]).wait()

    def next_g():
        step = min(64, m)

        def body(i, carry):
            here = pl.ds(pl.multiple_of(i * step, step), step)
            g_v[here, :] = acc_v[here, :].astype(BF16)
            acc_v[here, :] = g_v[here, :].astype(F32)
            return carry

        lax.fori_loop(0, m // step, body, 0)

    load_h(layers - 1)
    u_copy(0).start()
    tiles_total = TILES * (4 * (layers - 1) + 1)
    groups = 4 * (layers - 1) + 1

    def layer(tau, carry):
        l = layers - 1 - tau
        down, up = 2 * tau, 2 * tau + 1
        room_down, room_up = room(down), room(up)
        load_a(l).wait()

        @pl.when(tau > 0)
        def _():
            settle(down - 2, gd_ref)

        def product(room_j, lhs, rhs, base):
            def body(i, carry):
                cols = at(lax.rem(i + 1 + me.core, 2) * broad, broad)
                sums[room_j, cols, :] = dot_rows(lhs[:, cols], rhs[...])
                at_place(tau, base + i, (base, base + 1))
                return carry

            lax.fori_loop(0, 2, body, 0)

        product(room_down, a_v, g_v, 0)

        @pl.when(l > 0)
        def _():
            load_a(l - 1).start()

        def step(n, carry):
            k = 4 * TILES * tau + n
            block, slot = 4 * tau + lax.div(n, TILES), lax.rem(k, 2)
            ws = lax.rem(block, 2)
            here = pl.ds(pl.multiple_of(lax.rem(n, TILES) * tm, tm), tm)

            @pl.when(k + 1 < tiles_total)
            def _():
                u_copy(k + 1).start()

            @pl.when(lax.rem(n, TILES) == 0)
            def _():
                @pl.when(block + 1 < groups)
                def _():
                    load_w(block + 1)

                wait_w(block)

            u_copy(k).wait()
            few = tm // PARTS_BACKWARD
            for r in range(0, tm, few):
                some = pl.ds(pl.multiple_of(lax.rem(n, TILES) * tm + r, few), few)
                for j in range(0, d, wide):
                    da = dot_cols(g_v[some, :], w_v[ws, 1, j:j + wide, :])
                    v = u_v[slot, r:r + few, j:j + wide].astype(F32)
                    v2 = v * v
                    th = jnp.tanh(v * (K0 + K1 * v2))
                    slope = (1.0 + th) * (0.5 + (v * (1.0 - th)) * ((0.5 * K0) + (1.5 * K1) * v2))
                    d_v[some, j:j + wide] = (da * slope).astype(BF16)
            place = 2 * n + jnp.where(n >= TILES, 4, 2)
            at_place(tau, place, [2, 4] + list(range(8, 20, 2)))

            @pl.when(l > 0)
            def _():
                for j in range(0, d, wide):
                    acc_v[here, j:j + wide] += dot_cols(d_v[here, :], w_v[ws, 0, j:j + wide, :])

            at_place(tau, place + 1, [3, 5] + list(range(9, 20, 2)))

            @pl.when(n == TILES - 1)
            def _():
                pltpu.make_async_copy(x_ref, h_v, h_sem).wait()

                @pl.when(tau >= 2)
                def _():
                    settle(up - 4, gu_ref)

                product(room_up, h_v, d_v, 6)

                @pl.when(l > 0)
                def _():
                    load_h(l - 1)

            return carry

        lax.fori_loop(0, jnp.where(l > 0, 4 * TILES, TILES), step, 0)

        @pl.when(l > 0)
        def _():
            next_g()
            at_place(tau, 20, (20,))

        return carry

    lax.fori_loop(0, layers, layer, 0)
    for p, k, j in plan:
        if p >= 32 * layers:
            run(k, j)
    for j in range(2 * layers):
        ref = gd_ref if j % 2 == 0 else gu_ref
        finish(j, ref)
        if j >= 2 * layers - 3 and j != 2 * layers - 4:
            settle(j, ref)


def kernel(
    layers, total, x_ref, t_ref, up_ref, down_ref, w_ref, u_ref, a_ref, h_ref, gu_ref, gd_ref,
    h_v, y_v, t_v, w_v, u_v, act_v, d_v, a_v, sums, in1, in2, in3,
    w_sem, u_sem, act_sem, h_sem, t_sem, back_u_sem, back_a_sem, back_h_sem, out_sem, free1, *sems,
):
    def load_a(l):
        return pltpu.make_async_copy(a_ref.at[l], a_v, back_a_sem)

    def load_w(i):
        l, s = layers - 1 - lax.div(i, 4), lax.rem(i, 4)
        ws = lax.rem(i, 2)

        @pl.when(s == 0)
        def _():
            pltpu.make_async_copy(up_ref.at[l], w_v.at[ws, 0], w_sem.at[ws, 0]).start()
            pltpu.make_async_copy(down_ref.at[l], w_v.at[ws, 1], w_sem.at[ws, 1]).start()

        @pl.when(s > 0)
        def _():
            c = 3 * l + s - 1
            for k in (0, 1):
                pltpu.make_async_copy(w_ref.at[c, k], w_v.at[ws, k], w_sem.at[ws, k]).start()

    def prefetch():
        load_a(layers - 1).start()
        load_w(0)

    drain = forward_pass(
        layers, total, prefetch, x_ref, t_ref, up_ref, down_ref, w_ref, u_ref, a_ref, h_ref,
        h_v, y_v, t_v, w_v, u_v, act_v, w_sem, u_sem, act_sem, h_sem, t_sem, *sems[:16],
    )
    backward_pass(
        layers, load_a, load_w, x_ref, h_ref, up_ref, u_ref, gu_ref, gd_ref,
        h_v, y_v, w_v, u_v, d_v, a_v, t_v, sums, in1, in2, in3,
        w_sem, back_u_sem, back_h_sem, out_sem, free1, *sems[16:],
    )
    drain()


def any_specs(count):
    return [pl.BlockSpec(memory_space=pl.ANY)] * count


def local_step(hidden, targets, w_up, w_down, total_tokens):
    layers, d, own = w_up.shape
    m = hidden.shape[0]
    tm = m // TILES
    groups = 3 * layers
    dma = pltpu.SemaphoreType.DMA
    out = pl.pallas_call(
        functools.partial(kernel, layers, float(total_tokens)),
        out_shape=[
            jax.ShapeDtypeStruct((groups, 2, d, own), BF16),
            jax.ShapeDtypeStruct((4 * layers, m, own), BF16),
            jax.ShapeDtypeStruct((layers, m, own), BF16),
            jax.ShapeDtypeStruct((layers - 1, m, d), BF16),
            jax.ShapeDtypeStruct((layers, d, own), F32),
            jax.ShapeDtypeStruct((layers, own, d), F32),
        ],
        in_specs=any_specs(4),
        out_specs=any_specs(6),
        scratch_shapes=[
            pltpu.VMEM((m, d), BF16),
            pltpu.VMEM((m, d), F32),
            pltpu.VMEM((m, d), BF16),
            pltpu.VMEM((2, 2, d, own), BF16),
            pltpu.VMEM((2, tm, own), BF16),
            pltpu.VMEM((2, tm, own), BF16),
            pltpu.VMEM((m, own), BF16),
            pltpu.VMEM((m, own), BF16),
            pltpu.VMEM((3, d, own), F32),
            pltpu.VMEM((2, d // 2, own), F32),
            pltpu.VMEM((2, 2, d // 8, own), F32),
            pltpu.VMEM((2, 2, d // 16, own), F32),
            dma((2, 2)), dma((2,)), dma((2,)), dma((TILES,)), dma((2,)),
            dma((2,)), dma, dma, dma((2, 2)), pltpu.SemaphoreType.REGULAR,
        ] + [dma((groups,))] * 16 + [dma((2 * layers,))] * 2 + [dma((2, 2 * layers))] * 8 + [dma((2 * layers,))] * 2,
        compiler_params=pltpu.CompilerParams(collective_id=0, has_side_effects=True, vmem_limit_bytes=66_900_000),
        name="gradients",
    )(hidden, targets, w_up, w_down)
    return out[4], out[5]


def solution(mesh):
    def grad_step(hidden_in, targets, w_up, w_down):
        step_fn = functools.partial(local_step, total_tokens=hidden_in.shape[0])
        mapped = jax.shard_map(step_fn, mesh=mesh, in_specs=(P("dp", None), P("dp", None), P(None, None, "tp"), P(None, "tp", None)), out_specs=(P(None, None, "tp"), P(None, "tp", None)), check_vma=False)
        return mapped(hidden_in, targets, w_up, w_down)

    return grad_step
```

```python
import functools
import math
import jax
import jax.numpy as jnp
from jax import lax
from jax.experimental import pallas as pl
from jax.experimental.pallas import tpu as pltpu
from jax.sharding import PartitionSpec as P

BF16 = jnp.bfloat16
F32 = jnp.float32
MESH = pl.DeviceIdType.MESH
TILES = 2
PARTS_FORWARD = 8
PARTS_BACKWARD = 4
K0 = math.sqrt(2.0 / math.pi)
K1 = 0.044715 * K0
BY_ROWS = (((0,), (0,)), ((), ()))
BY_COLS = (((1,), (1,)), ((), ()))


def dot_cols(lhs, rhs):
    return lax.dot_general(lhs, rhs, BY_COLS, preferred_element_type=F32)


def dot_rows(lhs, rhs):
    return lax.dot_general(lhs, rhs, BY_ROWS, preferred_element_type=F32)


class Place:
    def __init__(self):
        z = lax.axis_index("tp")
        d = lax.axis_index("dp")
        self.core = lax.rem(d, 2)
        self.x = lax.rem(lax.div(d, 2), 2)
        self.y = lax.div(d, 4)
        self.inner = (z == 1) | (z == 2)
        self.near = {"tp": z + 1 - 2 * lax.rem(z, 2)}
        self.middle = {"tp": 3 - z}
        self.x_dev = {"dp": self.index(self.y, 1 - self.x, self.core)}
        self.y_dev = {"dp": self.index(1 - self.y, self.x, self.core)}
        self.partner = {"dp": self.index(self.y, self.x, 1 - self.core)}

    @staticmethod
    def index(y, x, core):
        return y * 4 + x * 2 + core


def remote(src, dst, send_sem, recv_sem, device):
    return pltpu.make_async_remote_copy(src_ref=src, dst_ref=dst, send_sem=send_sem, recv_sem=recv_sem, device_id=device, device_id_type=MESH)


def meet(devices):
    barrier = pltpu.get_barrier_semaphore()
    for device in devices:
        pl.semaphore_signal(barrier, inc=1, device_id=device, device_id_type=MESH)
    pl.semaphore_wait(barrier, len(devices))


FORWARD_TIMES = {
    "F": (0, 0, 0, 3, 4, 7, 16, 14, 22, 24, 26, 31),
    "Z": (2, 8, 17),
    "1": (0, 0, 2, 7, 8, 14, 20, 23, 32, 38, 39, 49),
    "2": (2, 4, 5, 13, 16, 20, 27, 30, 37, 46, 47, 54),
    "3": (3, 6, 8, 16, 21, 23, 32, 33, 41, 49, 53, 57),
    "L": (3, 7, 9, 14, 18, 22, 24, 29, 34, 35, 42, 45, 50, 54, 58),
}

BACKWARD_TIMES = (
    (0, 6, 32, 38, 64, 70, 96, 102),
    (2, 8, 34, 40, 66, 71, 98, 103),
    (7, 13, 41, 44, 74, 75, 128, 128),
    (11, 17, 46, 47, 77, 79, 131, 132),
    (15, 33, 49, 51, 80, 82, 133, 134),
    (83, 76, 148, 81, 103, 133, 137, 148),
    (99, 103, 151, 135, 143, 138, 151, 149),
)


def forward_plan():
    events = []
    for rank, (kind, times) in enumerate(FORWARD_TIMES.items()):
        for i, n in enumerate(times):
            c = i + 1 if kind in "ZL" else i
            age = 3 * c - 2.5 if kind == "Z" else c if kind != "L" else 3 * (c // 4) + (c % 4 - 1 if c % 4 else -0.5)
            events.append((n, age, rank, kind, c))
    return [(n, kind, c) for n, _, _, kind, c in sorted(events)]


def backward_plan():
    return [(p, k, j) for p, j, k in sorted((p, j, k + 1) for k, times in enumerate(BACKWARD_TIMES) for j, p in enumerate(times))]


def at_step(plan, now, block, steps, run):
    for b in sorted({e[0] // block for e in plan}):
        here = [e for e in plan if e[0] // block == b and e[0] % block in steps]
        if not here:
            continue

        @pl.when(lax.div(now, block) == b)
        def _():
            for n in sorted({e[0] for e in here}):
                @pl.when(now == n)
                def _():
                    for e in here:
                        if e[0] == n:
                            run(e[1], e[2])


def forward_pass(
    layers, total, prefetch, x_ref, t_ref, up_ref, down_ref, w_ref, u_ref, a_ref, h_ref,
    h_v, y_v, t_v, w_v, u_v, a_v, w_sem, u_sem, a_sem, h_sem, t_sem,
    zs, zr, fs, ms, mr, mf, xs, xr, ys, yr, as_, ar, bs, br, ds, dr,
):
    plan = forward_plan()
    me = Place()
    groups = 3 * layers
    m, d = h_v.shape
    tm = m // TILES
    part = d // 8
    half = part // 2
    last_n = 4 * TILES * layers - 1
    wide = min(256, d)

    def rows(y, x, core):
        return pl.multiple_of(core * (4 * part) + (y * 2 + x) * part, part)

    def square(core):
        return [rows(y, x, core) for y, x in ((me.y, me.x), (me.y, 1 - me.x), (1 - me.y, me.x), (1 - me.y, 1 - me.x))]

    ours, partners = square(me.core), square(1 - me.core)
    mine, of_x, of_y, of_d = ours

    def piece(c, start, size):
        return w_ref.at[c, :, pl.ds(start, size), :]

    def more(c):
        return d // 64 if c >= 3 else 0

    def z_rows(c):
        return [(mine, part, zs, zr, fs)] + ([(of_d + half - more(c), 2 * more(c), ms, mr, mf)] if more(c) else [])

    def z_copies(c):
        return [remote(piece(c, start, size), piece(c, start, size), send.at[c], recv.at[c], me.near) for start, size, send, recv, _ in z_rows(c)]

    def f_copies(c):
        to, device = (c + 2, me.middle) if c % 3 == 0 else (c, me.near)
        return [remote(piece(c, start, size), piece(to, start, size), send.at[c], recv.at[to], device) for start, size, _, recv, send in z_rows(c)]

    def x_copy(c, start):
        return remote(piece(c, start, part), piece(c, start, part), xs.at[c], xr.at[c], me.x_dev)

    def y_copy(c, start):
        return remote(piece(c, start, part), piece(c, start, part), ys.at[c], yr.at[c], me.y_dev)

    def a_copy(c, start):
        size = half - more(c)
        return remote(piece(c, start, size), piece(c, start, size), as_.at[c], ar.at[c], me.y_dev)

    def b_copy(c, start):
        start, size = start + half + more(c), half - more(c)
        return remote(piece(c, start, size), piece(c, start, size), bs.at[c], br.at[c], me.x_dev)

    def d_copy(c, i, starts):
        there = piece(c, starts[i], part)
        return remote(there, there, ds.at[i, c], dr.at[i, c], me.partner)

    def send_own(l, c, device):
        for start, size, send, recv, _ in z_rows(c):
            for k, own in enumerate((up_ref, down_ref)):
                there = w_ref.at[c, k, pl.ds(start, size), :]
                remote(own.at[l, pl.ds(start, size), :], there, send.at[c], recv.at[c], device).start()

    def load_w(g):
        l, s, ws = g // 4, g % 4, g % 2
        c = 3 * l + s - 1
        if s > 0:
            for i in range(4):
                d_copy(c, i, partners).wait_recv()
        for k, own in enumerate((up_ref, down_ref)):
            pltpu.make_async_copy(own.at[l] if s == 0 else w_ref.at[c, k], w_v.at[ws, k], w_sem.at[ws, k]).start()

    def run(kind, c):
        if kind == "Z":
            send_own(c, 3 * c, me.near)

            @pl.when(me.inner)
            def _():
                send_own(c, 3 * c + 1, me.middle)
        elif kind == "F":
            @pl.when(me.inner)
            def _():
                for copy in z_copies(c):
                    copy.wait_recv()
                for copy in f_copies(c):
                    copy.start()
        elif kind == "1":
            @pl.when(jnp.logical_not(me.inner))
            def _():
                for copy in z_copies(c):
                    copy.wait_recv()

            x_copy(c, mine).start()
            y_copy(c, mine).start()
            d_copy(c, 0, ours).start()
        elif kind == "2":
            x_copy(c, of_x).wait_recv()
            a_copy(c, of_x).start()
            y_copy(c, of_y).wait_recv()
            b_copy(c, of_y).start()
            d_copy(c, 1, ours).start()
            d_copy(c, 2, ours).start()
        elif kind == "3":
            a_copy(c, of_d).wait_recv()
            b_copy(c, of_d).wait_recv()
            d_copy(c, 3, ours).start()
        else:
            load_w(c)

    first = pltpu.make_async_copy(x_ref, h_v, t_sem.at[0])
    first.start()
    load_w(0)
    meet([me.near, me.middle, me.x_dev, me.y_dev, me.partner])
    run("Z", 0)
    last = pltpu.make_async_copy(t_ref, t_v, t_sem.at[1])
    last.start()
    y_v[...] = jnp.zeros_like(y_v)
    first.wait()

    def tile_of(n):
        return lax.rem(n, TILES)

    def there(n):
        return pl.ds(pl.multiple_of(tile_of(n) * tm, tm), tm)

    def slot_of(n):
        return lax.rem(lax.div(n, TILES), 2)

    def wait_w(n):
        for k in (0, 1):
            pltpu.make_async_copy(up_ref.at[0], w_v.at[slot_of(n), k], w_sem.at[slot_of(n), k]).wait()

    def u_copy(n):
        slot = lax.rem(n, 2)
        return pltpu.make_async_copy(u_v.at[slot], u_ref.at[lax.div(n, TILES), there(n), :], u_sem.at[slot])

    def a_out(n):
        slot = lax.rem(n, 2)
        return pltpu.make_async_copy(a_v.at[slot], a_ref.at[lax.div(n, 4 * TILES), there(n), :], a_sem.at[slot])

    def h_out(dst, n):
        return pltpu.make_async_copy(h_v.at[there(n), :], dst.at[there(n), :], h_sem.at[tile_of(n)])

    def is_block(n, s):
        return lax.rem(lax.div(n, TILES), 4) == s

    def settle_rows(n):
        l = lax.div(n, 4 * TILES)

        @pl.when(l > 0)
        def _():
            h_out(h_ref.at[0], n).wait()

        def sweep(last_layer):
            size = min(32, tm)

            def body(i, carry):
                few = pl.ds(pl.multiple_of(tile_of(n) * tm + i * size, size), size)
                h_new = (h_v[few, :].astype(F32) + y_v[few, :].astype(BF16).astype(F32)).astype(BF16)
                if last_layer:
                    h_new = ((h_new.astype(F32) - t_v[few, :].astype(F32)) / total).astype(BF16)
                h_v[few, :] = h_new
                y_v[few, :] = h_new.astype(F32) if last_layer else jnp.zeros((size, d), F32)
                return carry

            lax.fori_loop(0, tm // size, body, 0)

        @pl.when(l < layers - 1)
        def _():
            sweep(False)
            h_out(h_ref.at[l], n).start()

        @pl.when(l == layers - 1)
        def _():
            sweep(True)

    def step(n, carry):
        here, slot, ws = there(n), lax.rem(n, 2), slot_of(n)

        @pl.when(n >= 2)
        def _():
            u_copy(n).wait()

        @pl.when((n >= 2) & is_block(n - 2, 0))
        def _():
            a_out(n).wait()

        @pl.when(tile_of(n) == 0)
        def _():
            wait_w(n)

        few = tm // PARTS_FORWARD
        for r in range(0, tm, few):
            some = pl.ds(pl.multiple_of(tile_of(n) * tm + r, few), few)
            for j in range(0, d, wide):
                u = jnp.dot(h_v[some, :], w_v[ws, 0, :, j:j + wide], preferred_element_type=F32).astype(BF16)
                u_v[slot, r:r + few, j:j + wide] = u
                v = u.astype(F32)
                th = jnp.tanh(v * (K0 + K1 * (v * v)))
                hv = 0.5 * v
                a_v[slot, r:r + few, j:j + wide] = (hv + hv * th).astype(BF16)
        u_copy(n).start()

        @pl.when(is_block(n, 0))
        def _():
            a_out(n).start()

        @pl.when(n == last_n - TILES + 1)
        def _():
            prefetch()

        at_step(plan, 2 * n, 8 * TILES, range(0, 8 * TILES, 2), run)
        for j in range(0, d, wide):
            y_v[here, j:j + wide] += jnp.dot(a_v[slot], w_v[ws, 1, :, j:j + wide], preferred_element_type=F32)

        @pl.when(is_block(n, 3))
        def _():
            settle_rows(n)

        at_step(plan, 2 * n + 1, 8 * TILES, range(1, 8 * TILES, 2), run)

        return carry

    last.wait()
    lax.fori_loop(0, last_n + 1, step, 0)
    u_copy(last_n - 1).wait()
    u_copy(last_n).wait()

    def drain():
        for c in range(groups):
            if c % 3 == 0:
                for copy in z_copies(c):
                    copy.wait_send()

            @pl.when(me.inner)
            def _():
                for copy in f_copies(c) + (z_copies(c) if c % 3 == 1 else []):
                    copy.wait_send()

            x_copy(c, mine).wait_send()
            y_copy(c, mine).wait_send()
            a_copy(c, of_x).wait_send()
            b_copy(c, of_y).wait_send()
            for i in range(4):
                d_copy(c, i, ours).wait_send()

    return drain


def backward_pass(
    layers, load_a, load_w, x_ref, h_ref, up_ref, u_ref, gu_ref, gd_ref,
    g_v, acc_v, w_v, u_v, d_v, a_v, h_v, sums, in1, in2, in3,
    w_sem, u_sem, h_sem, out_sem, free1,
    s1, r1, s2, r2, s3, r3, s4, r4, s5, r5, s6, r6,
):
    plan = backward_plan()
    me = Place()
    m, d = g_v.shape
    tm = m // TILES
    hd, qd = d // 2, d // 4
    e8, e16 = d // 8, d // 16
    wide = min(256, d)
    broad = d // 2

    def at(value, size):
        return pl.ds(pl.multiple_of(value, size), size)

    own = me.core * hd
    own_rows, other_rows = at(own, hd), at(hd - own, hd)
    a_base, b_base = own, own + qd
    a_keep, a_give = at(a_base + me.x * e8, e8), at(a_base + (1 - me.x) * e8, e8)
    b_keep, b_give = at(b_base + me.y * e8, e8), at(b_base + (1 - me.y) * e8, e8)
    a_last, a_pass = at(a_base + me.x * e8 + me.y * e16, e16), at(a_base + me.x * e8 + (1 - me.y) * e16, e16)
    b_last, b_pass = at(b_base + me.y * e8 + me.x * e16, e16), at(b_base + me.y * e8 + (1 - me.x) * e16, e16)

    def room(j):
        return lax.rem(j, 2) * (1 + lax.rem(lax.div(j, 2), 2))

    def c1(j):
        return remote(sums.at[room(j), other_rows, :], in1.at[lax.rem(j, 2)], s1.at[j], r1.at[j], me.partner)

    def c2(j):
        q, r = room(j), lax.rem(j, 2)
        return (remote(sums.at[q, a_give, :], in2.at[r, 0], s2.at[0, j], r2.at[0, j], me.x_dev),
                remote(sums.at[q, b_give, :], in2.at[r, 1], s2.at[1, j], r2.at[1, j], me.y_dev))

    def c3(j):
        q, r = room(j), lax.rem(j, 2)
        return (remote(sums.at[q, a_pass, :], in3.at[r, 0], s3.at[0, j], r3.at[0, j], me.y_dev),
                remote(sums.at[q, b_pass, :], in3.at[r, 1], s3.at[1, j], r3.at[1, j], me.x_dev))

    def c4(j, ref, a_rows, b_rows):
        q, dst = room(j), ref.at[layers - 1 - lax.div(j, 2)]
        return (remote(sums.at[q, a_rows, :], dst.at[a_rows, :], s4.at[0, j], r4.at[0, j], me.y_dev),
                remote(sums.at[q, b_rows, :], dst.at[b_rows, :], s4.at[1, j], r4.at[1, j], me.x_dev))

    def keep(j, ref):
        q, dst = room(j), ref.at[layers - 1 - lax.div(j, 2)]
        return (pltpu.make_async_copy(sums.at[q, a_last, :], dst.at[a_last, :], out_sem.at[0, lax.rem(j, 2)]),
                pltpu.make_async_copy(sums.at[q, b_last, :], dst.at[b_last, :], out_sem.at[1, lax.rem(j, 2)]))

    def c5(j, ref, a_rows, b_rows):
        dst = ref.at[layers - 1 - lax.div(j, 2)]
        return (remote(dst.at[a_rows, :], dst.at[a_rows, :], s5.at[0, j], r5.at[0, j], me.x_dev),
                remote(dst.at[b_rows, :], dst.at[b_rows, :], s5.at[1, j], r5.at[1, j], me.y_dev))

    def c6(j, ref, which):
        dst = ref.at[layers - 1 - lax.div(j, 2)]
        return remote(dst.at[which, :], dst.at[which, :], s6.at[j], r6.at[j], me.partner)

    def add(j, start, size, buffer):
        q = room(j)
        step = min(32, size)

        def body(i, carry):
            there = pl.ds(pl.multiple_of(start + i * step, step), step)
            sums[q, there, :] = sums[q, there, :] + buffer[pl.ds(pl.multiple_of(i * step, step), step), :]
            return carry

        lax.fori_loop(0, size // step, body, 0)

    def step1(j):
        @pl.when(j >= 2)
        def _():
            pl.semaphore_wait(free1, 1)

        c1(j).start()

    def step2(j):
        c1(j).wait_recv()
        add(j, own, hd, in1.at[lax.rem(j, 2)])

        @pl.when(j < 2 * layers - 2)
        def _():
            pl.semaphore_signal(free1, inc=1, device_id=me.partner, device_id_type=MESH)

        for copy in c2(j):
            copy.start()

    def step3(j):
        r, got, put = lax.rem(j, 2), c2(j), c3(j)
        for k, start in enumerate((a_base + me.x * e8, b_base + me.y * e8)):
            got[k].wait_recv()
            add(j, start, e8, in2.at[r, k])
            put[k].start()

    def step4(j, ref):
        r, got, put, local = lax.rem(j, 2), c3(j), c4(j, ref, a_last, b_last), keep(j, ref)
        for k, start in enumerate((a_base + me.x * e8 + me.y * e16, b_base + me.y * e8 + me.x * e16)):
            got[k].wait_recv()
            add(j, start, e16, in3.at[r, k])
            put[k].start()
            local[k].start()

    def step5(j, ref):
        got, put, local = c4(j, ref, a_pass, b_pass), c5(j, ref, a_keep, b_keep), keep(j, ref)
        for k in (0, 1):
            local[k].wait()
            got[k].wait_recv()
            put[k].start()

    def step6(j, ref):
        for copy in c5(j, ref, a_give, b_give):
            copy.wait_recv()
        c6(j, ref, own_rows).start()

    def step7(j, ref):
        c6(j, ref, other_rows).wait_recv()

    def settle(j, ref):
        c1(j).wait_send()
        for copy in c2(j) + c3(j) + c4(j, ref, a_last, b_last):
            copy.wait_send()

    def finish(j, ref):
        for copy in c5(j, ref, a_keep, b_keep):
            copy.wait_send()
        c6(j, ref, own_rows).wait_send()

    def run(k, j):
        ref = gd_ref if j % 2 == 0 else gu_ref
        (step1, step2, step3, step4, step5, step6, step7)[k - 1](*((j,) if k <= 3 else (j, ref)))

    def at_place(tau, p, steps):
        at_step(plan, 32 * tau + p, 32, steps, run)

    def u_copy(n):
        l, s, t, slot = layers - 1 - lax.div(n, 4 * TILES), lax.rem(lax.div(n, TILES), 4), lax.rem(n, TILES), lax.rem(n, 2)
        return pltpu.make_async_copy(u_ref.at[4 * l + s, pl.ds(t * tm, tm), :], u_v.at[slot], u_sem.at[slot])

    def load_h(l):
        @pl.when(l == 0)
        def _():
            pltpu.make_async_copy(x_ref, h_v, h_sem).start()

        @pl.when(l > 0)
        def _():
            pltpu.make_async_copy(h_ref.at[l - 1], h_v, h_sem).start()

    def wait_w(i):
        for k in (0, 1):
            pltpu.make_async_copy(up_ref.at[0], w_v.at[lax.rem(i, 2), k], w_sem.at[lax.rem(i, 2), k]).wait()

    def next_g():
        step = min(64, m)

        def body(i, carry):
            here = pl.ds(pl.multiple_of(i * step, step), step)
            g_v[here, :] = acc_v[here, :].astype(BF16)
            acc_v[here, :] = g_v[here, :].astype(F32)
            return carry

        lax.fori_loop(0, m // step, body, 0)

    load_h(layers - 1)
    u_copy(0).start()
    tiles_total = TILES * (4 * (layers - 1) + 1)
    groups = 4 * (layers - 1) + 1

    def layer(tau, carry):
        l = layers - 1 - tau
        down, up = 2 * tau, 2 * tau + 1
        room_down, room_up = room(down), room(up)
        load_a(l).wait()

        @pl.when(tau > 0)
        def _():
            settle(down - 2, gd_ref)

        def product(room_j, lhs, rhs, base):
            def body(i, carry):
                cols = at(lax.rem(i + 1 + me.core, 2) * broad, broad)
                sums[room_j, cols, :] = dot_rows(lhs[:, cols], rhs[...])
                at_place(tau, base + i, (base, base + 1))
                return carry

            lax.fori_loop(0, 2, body, 0)

        product(room_down, a_v, g_v, 0)

        @pl.when(l > 0)
        def _():
            load_a(l - 1).start()

        def step(n, carry):
            k = 4 * TILES * tau + n
            block, slot = 4 * tau + lax.div(n, TILES), lax.rem(k, 2)
            ws = lax.rem(block, 2)
            here = pl.ds(pl.multiple_of(lax.rem(n, TILES) * tm, tm), tm)

            @pl.when(k + 1 < tiles_total)
            def _():
                u_copy(k + 1).start()

            @pl.when(lax.rem(n, TILES) == 0)
            def _():
                @pl.when(block + 1 < groups)
                def _():
                    load_w(block + 1)

                wait_w(block)

            u_copy(k).wait()
            few = tm // PARTS_BACKWARD
            for r in range(0, tm, few):
                some = pl.ds(pl.multiple_of(lax.rem(n, TILES) * tm + r, few), few)
                for j in range(0, d, wide):
                    da = dot_cols(g_v[some, :], w_v[ws, 1, j:j + wide, :])
                    v = u_v[slot, r:r + few, j:j + wide].astype(F32)
                    v2 = v * v
                    th = jnp.tanh(v * (K0 + K1 * v2))
                    slope = (1.0 + th) * (0.5 + (v * (1.0 - th)) * ((0.5 * K0) + (1.5 * K1) * v2))
                    d_v[some, j:j + wide] = (da * slope).astype(BF16)
            place = 2 * n + jnp.where(n >= TILES, 4, 2)
            at_place(tau, place, [2, 4] + list(range(8, 20, 2)))

            @pl.when(l > 0)
            def _():
                for j in range(0, d, wide):
                    acc_v[here, j:j + wide] += dot_cols(d_v[here, :], w_v[ws, 0, j:j + wide, :])

            at_place(tau, place + 1, [3, 5] + list(range(9, 20, 2)))

            @pl.when(n == TILES - 1)
            def _():
                pltpu.make_async_copy(x_ref, h_v, h_sem).wait()

                @pl.when(tau >= 2)
                def _():
                    settle(up - 4, gu_ref)

                product(room_up, h_v, d_v, 6)

                @pl.when(l > 0)
                def _():
                    load_h(l - 1)

            return carry

        lax.fori_loop(0, jnp.where(l > 0, 4 * TILES, TILES), step, 0)

        @pl.when(l > 0)
        def _():
            next_g()
            at_place(tau, 20, (20,))

        return carry

    lax.fori_loop(0, layers, layer, 0)
    for p, k, j in plan:
        if p >= 32 * layers:
            run(k, j)
    for j in range(2 * layers):
        ref = gd_ref if j % 2 == 0 else gu_ref
        finish(j, ref)
        if j >= 2 * layers - 3 and j != 2 * layers - 4:
            settle(j, ref)


def kernel(
    layers, total, x_ref, t_ref, up_ref, down_ref, w_ref, u_ref, a_ref, h_ref, gu_ref, gd_ref,
    h_v, y_v, t_v, w_v, u_v, act_v, d_v, a_v, sums, in1, in2, in3,
    w_sem, u_sem, act_sem, h_sem, t_sem, back_u_sem, back_a_sem, back_h_sem, out_sem, free1, *sems,
):
    def load_a(l):
        return pltpu.make_async_copy(a_ref.at[l], a_v, back_a_sem)

    def load_w(i):
        l, s = layers - 1 - lax.div(i, 4), lax.rem(i, 4)
        ws = lax.rem(i, 2)

        @pl.when(s == 0)
        def _():
            pltpu.make_async_copy(up_ref.at[l], w_v.at[ws, 0], w_sem.at[ws, 0]).start()
            pltpu.make_async_copy(down_ref.at[l], w_v.at[ws, 1], w_sem.at[ws, 1]).start()

        @pl.when(s > 0)
        def _():
            c = 3 * l + s - 1
            for k in (0, 1):
                pltpu.make_async_copy(w_ref.at[c, k], w_v.at[ws, k], w_sem.at[ws, k]).start()

    def prefetch():
        load_a(layers - 1).start()
        load_w(0)

    drain = forward_pass(
        layers, total, prefetch, x_ref, t_ref, up_ref, down_ref, w_ref, u_ref, a_ref, h_ref,
        h_v, y_v, t_v, w_v, u_v, act_v, w_sem, u_sem, act_sem, h_sem, t_sem, *sems[:16],
    )
    backward_pass(
        layers, load_a, load_w, x_ref, h_ref, up_ref, u_ref, gu_ref, gd_ref,
        h_v, y_v, w_v, u_v, d_v, a_v, t_v, sums, in1, in2, in3,
        w_sem, back_u_sem, back_h_sem, out_sem, free1, *sems[16:],
    )
    drain()


def any_specs(count):
    return [pl.BlockSpec(memory_space=pl.ANY)] * count


def local_step(hidden, targets, w_up, w_down, total_tokens):
    layers, d, own = w_up.shape
    m = hidden.shape[0]
    tm = m // TILES
    groups = 3 * layers
    dma = pltpu.SemaphoreType.DMA
    out = pl.pallas_call(
        functools.partial(kernel, layers, float(total_tokens)),
        out_shape=[
            jax.ShapeDtypeStruct((groups, 2, d, own), BF16),
            jax.ShapeDtypeStruct((4 * layers, m, own), BF16),
            jax.ShapeDtypeStruct((layers, m, own), BF16),
            jax.ShapeDtypeStruct((layers - 1, m, d), BF16),
            jax.ShapeDtypeStruct((layers, d, own), F32),
            jax.ShapeDtypeStruct((layers, own, d), F32),
        ],
        in_specs=any_specs(4),
        out_specs=any_specs(6),
        scratch_shapes=[
            pltpu.VMEM((m, d), BF16),
            pltpu.VMEM((m, d), F32),
            pltpu.VMEM((m, d), BF16),
            pltpu.VMEM((2, 2, d, own), BF16),
            pltpu.VMEM((2, tm, own), BF16),
            pltpu.VMEM((2, tm, own), BF16),
            pltpu.VMEM((m, own), BF16),
            pltpu.VMEM((m, own), BF16),
            pltpu.VMEM((3, d, own), F32),
            pltpu.VMEM((2, d // 2, own), F32),
            pltpu.VMEM((2, 2, d // 8, own), F32),
            pltpu.VMEM((2, 2, d // 16, own), F32),
            dma((2, 2)), dma((2,)), dma((2,)), dma((TILES,)), dma((2,)),
            dma((2,)), dma, dma, dma((2, 2)), pltpu.SemaphoreType.REGULAR,
        ] + [dma((groups,))] * 14 + [dma((4, groups))] * 2 + [dma((2 * layers,))] * 2 + [dma((2, 2 * layers))] * 8 + [dma((2 * layers,))] * 2,
        compiler_params=pltpu.CompilerParams(collective_id=0, has_side_effects=True, vmem_limit_bytes=66_900_000),
        name="gradients",
    )(hidden, targets, w_up, w_down)
    return out[4], out[5]


def solution(mesh):
    def grad_step(hidden_in, targets, w_up, w_down):
        step_fn = functools.partial(local_step, total_tokens=hidden_in.shape[0])
        mapped = jax.shard_map(step_fn, mesh=mesh, in_specs=(P("dp", None), P("dp", None), P(None, None, "tp"), P(None, "tp", None)), out_specs=(P(None, None, "tp"), P(None, "tp", None)), check_vma=False)
        return mapped(hidden_in, targets, w_up, w_down)

    return grad_step
```

```python
import functools
import math
import jax
import jax.numpy as jnp
from jax import lax
from jax.experimental import pallas as pl
from jax.experimental.pallas import tpu as pltpu
from jax.sharding import PartitionSpec as P

BF16 = jnp.bfloat16
F32 = jnp.float32
MESH = pl.DeviceIdType.MESH
TILES = 2
PARTS_FORWARD = 8
PARTS_BACKWARD = 4
K0 = math.sqrt(2.0 / math.pi)
K1 = 0.044715 * K0
BY_ROWS = (((0,), (0,)), ((), ()))
BY_COLS = (((1,), (1,)), ((), ()))


def dot_cols(lhs, rhs):
    return lax.dot_general(lhs, rhs, BY_COLS, preferred_element_type=F32)


def dot_rows(lhs, rhs):
    return lax.dot_general(lhs, rhs, BY_ROWS, preferred_element_type=F32)


class Place:
    def __init__(self):
        z = lax.axis_index("tp")
        d = lax.axis_index("dp")
        self.core = lax.rem(d, 2)
        self.x = lax.rem(lax.div(d, 2), 2)
        self.y = lax.div(d, 4)
        self.inner = (z == 1) | (z == 2)
        self.near = {"tp": z + 1 - 2 * lax.rem(z, 2)}
        self.middle = {"tp": 3 - z}
        self.x_dev = {"dp": self.index(self.y, 1 - self.x, self.core)}
        self.y_dev = {"dp": self.index(1 - self.y, self.x, self.core)}
        self.partner = {"dp": self.index(self.y, self.x, 1 - self.core)}

    @staticmethod
    def index(y, x, core):
        return y * 4 + x * 2 + core


def remote(src, dst, send_sem, recv_sem, device):
    return pltpu.make_async_remote_copy(src_ref=src, dst_ref=dst, send_sem=send_sem, recv_sem=recv_sem, device_id=device, device_id_type=MESH)


def meet(devices):
    barrier = pltpu.get_barrier_semaphore()
    for device in devices:
        pl.semaphore_signal(barrier, inc=1, device_id=device, device_id_type=MESH)
    pl.semaphore_wait(barrier, len(devices))


FORWARD_TIMES = {
    "F": (0, 0, 0, 3, 3, 6, 15, 16, 21, 30, 33, 36),
    "Z": (1, 8, 22),
    "1": (0, 0, 1, 5, 7, 12, 20, 23, 28, 35, 40, 44),
    "2": (1, 2, 4, 12, 17, 19, 26, 33, 35, 43, 48, 51),
    "3": (3, 5, 7, 15, 20, 22, 32, 36, 39, 47, 52, 54),
    "L": (3, 6, 9, 11, 18, 22, 25, 27, 34, 38, 41, 46, 50, 54, 56),
}

BACKWARD_TIMES = (
    (0, 6, 32, 38, 64, 70, 96, 102),
    (2, 8, 34, 40, 66, 71, 98, 103),
    (7, 13, 41, 44, 74, 75, 128, 128),
    (11, 17, 46, 47, 77, 79, 131, 132),
    (15, 33, 49, 51, 80, 82, 133, 134),
    (83, 76, 148, 81, 103, 133, 137, 148),
    (99, 103, 151, 135, 143, 138, 151, 149),
)


def forward_plan():
    events = []
    for rank, (kind, times) in enumerate(FORWARD_TIMES.items()):
        for i, n in enumerate(times):
            c = i + 1 if kind in "ZL" else i
            age = 3 * c - 2.5 if kind == "Z" else c if kind != "L" else 3 * (c // 4) + (c % 4 - 1 if c % 4 else -0.5)
            events.append((n, age, rank, kind, c))
    return [(n, kind, c) for n, _, _, kind, c in sorted(events)]


def backward_plan():
    return [(p, k, j) for p, j, k in sorted((p, j, k + 1) for k, times in enumerate(BACKWARD_TIMES) for j, p in enumerate(times))]


def at_step(plan, now, block, steps, run):
    for b in sorted({e[0] // block for e in plan}):
        here = [e for e in plan if e[0] // block == b and e[0] % block in steps]
        if not here:
            continue

        @pl.when(lax.div(now, block) == b)
        def _():
            for n in sorted({e[0] for e in here}):
                @pl.when(now == n)
                def _():
                    for e in here:
                        if e[0] == n:
                            run(e[1], e[2])


def forward_pass(
    layers, total, prefetch, x_ref, t_ref, up_ref, down_ref, w_ref, u_ref, a_ref, h_ref,
    h_v, y_v, t_v, w_v, u_v, a_v, w_sem, u_sem, a_sem, h_sem, t_sem,
    zs, zr, fs, ms, mr, mf, xs, xr, ys, yr, as_, ar, bs, br, ds, dr,
):
    plan = forward_plan()
    me = Place()
    groups = 3 * layers
    m, d = h_v.shape
    tm = m // TILES
    part = d // 8
    half = part // 2
    last_n = 4 * TILES * layers - 1
    wide = min(256, d)

    def rows(y, x):
        return pl.multiple_of(me.core * (4 * part) + (y * 2 + x) * part, part)

    mine, of_x, of_y, of_d = rows(me.y, me.x), rows(me.y, 1 - me.x), rows(1 - me.y, me.x), rows(1 - me.y, 1 - me.x)
    half_mine = pl.multiple_of(me.core * (4 * part), 4 * part)
    half_other = pl.multiple_of((1 - me.core) * (4 * part), 4 * part)

    def piece(c, start, size):
        return w_ref.at[c, :, pl.ds(start, size), :]

    def more(c):
        return d // 64 if c >= 3 else 0

    def z_rows(c):
        return [(mine, part, zs, zr, fs)] + ([(of_d + half - more(c), 2 * more(c), ms, mr, mf)] if more(c) else [])

    def z_copies(c):
        return [remote(piece(c, start, size), piece(c, start, size), send.at[c], recv.at[c], me.near) for start, size, send, recv, _ in z_rows(c)]

    def f_copies(c):
        to, device = (c + 2, me.middle) if c % 3 == 0 else (c, me.near)
        return [remote(piece(c, start, size), piece(to, start, size), send.at[c], recv.at[to], device) for start, size, _, recv, send in z_rows(c)]

    def x_copy(c, start):
        return remote(piece(c, start, part), piece(c, start, part), xs.at[c], xr.at[c], me.x_dev)

    def y_copy(c, start):
        return remote(piece(c, start, part), piece(c, start, part), ys.at[c], yr.at[c], me.y_dev)

    def a_copy(c, start):
        size = half - more(c)
        return remote(piece(c, start, size), piece(c, start, size), as_.at[c], ar.at[c], me.y_dev)

    def b_copy(c, start):
        start, size = start + half + more(c), half - more(c)
        return remote(piece(c, start, size), piece(c, start, size), bs.at[c], br.at[c], me.x_dev)

    def d_copy(c, start):
        return remote(piece(c, start, 4 * part), piece(c, start, 4 * part), ds.at[c], dr.at[c], me.partner)

    def send_own(l, c, device):
        for start, size, send, recv, _ in z_rows(c):
            for k, own in enumerate((up_ref, down_ref)):
                there = w_ref.at[c, k, pl.ds(start, size), :]
                remote(own.at[l, pl.ds(start, size), :], there, send.at[c], recv.at[c], device).start()

    def load_w(g):
        l, s, ws = g // 4, g % 4, g % 2
        c = 3 * l + s - 1
        if s > 0:
            d_copy(c, half_other).wait_recv()
        for k, own in enumerate((up_ref, down_ref)):
            pltpu.make_async_copy(own.at[l] if s == 0 else w_ref.at[c, k], w_v.at[ws, k], w_sem.at[ws, k]).start()

    def run(kind, c):
        if kind == "Z":
            send_own(c, 3 * c, me.near)

            @pl.when(me.inner)
            def _():
                send_own(c, 3 * c + 1, me.middle)
        elif kind == "F":
            @pl.when(me.inner)
            def _():
                for copy in z_copies(c):
                    copy.wait_recv()
                for copy in f_copies(c):
                    copy.start()
        elif kind == "1":
            @pl.when(jnp.logical_not(me.inner))
            def _():
                for copy in z_copies(c):
                    copy.wait_recv()

            x_copy(c, mine).start()
            y_copy(c, mine).start()
        elif kind == "2":
            x_copy(c, of_x).wait_recv()
            a_copy(c, of_x).start()
            y_copy(c, of_y).wait_recv()
            b_copy(c, of_y).start()
        elif kind == "3":
            a_copy(c, of_d).wait_recv()
            b_copy(c, of_d).wait_recv()
            d_copy(c, half_mine).start()
        else:
            load_w(c)

    first = pltpu.make_async_copy(x_ref, h_v, t_sem.at[0])
    first.start()
    load_w(0)
    meet([me.near, me.middle, me.x_dev, me.y_dev, me.partner])
    run("Z", 0)
    last = pltpu.make_async_copy(t_ref, t_v, t_sem.at[1])
    last.start()
    y_v[...] = jnp.zeros_like(y_v)
    first.wait()

    def tile_of(n):
        return lax.rem(n, TILES)

    def there(n):
        return pl.ds(pl.multiple_of(tile_of(n) * tm, tm), tm)

    def slot_of(n):
        return lax.rem(lax.div(n, TILES), 2)

    def wait_w(n):
        for k in (0, 1):
            pltpu.make_async_copy(up_ref.at[0], w_v.at[slot_of(n), k], w_sem.at[slot_of(n), k]).wait()

    def u_copy(n):
        slot = lax.rem(n, 2)
        return pltpu.make_async_copy(u_v.at[slot], u_ref.at[lax.div(n, TILES), there(n), :], u_sem.at[slot])

    def a_out(n):
        slot = lax.rem(n, 2)
        return pltpu.make_async_copy(a_v.at[slot], a_ref.at[lax.div(n, 4 * TILES), there(n), :], a_sem.at[slot])

    def h_out(dst, n):
        return pltpu.make_async_copy(h_v.at[there(n), :], dst.at[there(n), :], h_sem.at[tile_of(n)])

    def is_block(n, s):
        return lax.rem(lax.div(n, TILES), 4) == s

    def settle_rows(n):
        l = lax.div(n, 4 * TILES)

        @pl.when(l > 0)
        def _():
            h_out(h_ref.at[0], n).wait()

        def sweep(last_layer):
            size = min(32, tm)

            def body(i, carry):
                few = pl.ds(pl.multiple_of(tile_of(n) * tm + i * size, size), size)
                h_new = (h_v[few, :].astype(F32) + y_v[few, :].astype(BF16).astype(F32)).astype(BF16)
                if last_layer:
                    h_new = ((h_new.astype(F32) - t_v[few, :].astype(F32)) / total).astype(BF16)
                h_v[few, :] = h_new
                y_v[few, :] = h_new.astype(F32) if last_layer else jnp.zeros((size, d), F32)
                return carry

            lax.fori_loop(0, tm // size, body, 0)

        @pl.when(l < layers - 1)
        def _():
            sweep(False)
            h_out(h_ref.at[l], n).start()

        @pl.when(l == layers - 1)
        def _():
            sweep(True)

    def step(n, carry):
        here, slot, ws = there(n), lax.rem(n, 2), slot_of(n)

        @pl.when(n >= 2)
        def _():
            u_copy(n).wait()

        @pl.when((n >= 2) & is_block(n - 2, 0))
        def _():
            a_out(n).wait()

        @pl.when(tile_of(n) == 0)
        def _():
            wait_w(n)

        few = tm // PARTS_FORWARD
        for r in range(0, tm, few):
            some = pl.ds(pl.multiple_of(tile_of(n) * tm + r, few), few)
            for j in range(0, d, wide):
                u = jnp.dot(h_v[some, :], w_v[ws, 0, :, j:j + wide], preferred_element_type=F32).astype(BF16)
                u_v[slot, r:r + few, j:j + wide] = u
                v = u.astype(F32)
                th = jnp.tanh(v * (K0 + K1 * (v * v)))
                hv = 0.5 * v
                a_v[slot, r:r + few, j:j + wide] = (hv + hv * th).astype(BF16)
        u_copy(n).start()

        @pl.when(is_block(n, 0))
        def _():
            a_out(n).start()

        @pl.when(n == last_n - TILES + 1)
        def _():
            prefetch()

        at_step(plan, 2 * n, 8 * TILES, range(0, 8 * TILES, 2), run)
        for j in range(0, d, wide):
            y_v[here, j:j + wide] += jnp.dot(a_v[slot], w_v[ws, 1, :, j:j + wide], preferred_element_type=F32)

        @pl.when(is_block(n, 3))
        def _():
            settle_rows(n)

        at_step(plan, 2 * n + 1, 8 * TILES, range(1, 8 * TILES, 2), run)

        return carry

    last.wait()
    lax.fori_loop(0, last_n + 1, step, 0)
    u_copy(last_n - 1).wait()
    u_copy(last_n).wait()

    def drain():
        for c in range(groups):
            if c % 3 == 0:
                for copy in z_copies(c):
                    copy.wait_send()

            @pl.when(me.inner)
            def _():
                for copy in f_copies(c) + (z_copies(c) if c % 3 == 1 else []):
                    copy.wait_send()

            x_copy(c, mine).wait_send()
            y_copy(c, mine).wait_send()
            a_copy(c, of_x).wait_send()
            b_copy(c, of_y).wait_send()
            d_copy(c, half_mine).wait_send()

    return drain


def backward_pass(
    layers, load_a, load_w, x_ref, h_ref, up_ref, u_ref, gu_ref, gd_ref,
    g_v, acc_v, w_v, u_v, d_v, a_v, h_v, sums, in1, in2, in3,
    w_sem, u_sem, h_sem, out_sem, free1,
    s1, r1, s2, r2, s3, r3, s4, r4, s5, r5, s6, r6,
):
    plan = backward_plan()
    me = Place()
    m, d = g_v.shape
    tm = m // TILES
    hd, qd = d // 2, d // 4
    e8, e16 = d // 8, d // 16
    wide = min(256, d)
    broad = d // 2

    def at(value, size):
        return pl.ds(pl.multiple_of(value, size), size)

    own = me.core * hd
    own_rows, other_rows = at(own, hd), at(hd - own, hd)
    a_base, b_base = own, own + qd
    a_keep, a_give = at(a_base + me.x * e8, e8), at(a_base + (1 - me.x) * e8, e8)
    b_keep, b_give = at(b_base + me.y * e8, e8), at(b_base + (1 - me.y) * e8, e8)
    a_last, a_pass = at(a_base + me.x * e8 + me.y * e16, e16), at(a_base + me.x * e8 + (1 - me.y) * e16, e16)
    b_last, b_pass = at(b_base + me.y * e8 + me.x * e16, e16), at(b_base + me.y * e8 + (1 - me.x) * e16, e16)

    def room(j):
        return lax.rem(j, 2) * (1 + lax.rem(lax.div(j, 2), 2))

    def c1(j):
        return remote(sums.at[room(j), other_rows, :], in1.at[lax.rem(j, 2)], s1.at[j], r1.at[j], me.partner)

    def c2(j):
        q, r = room(j), lax.rem(j, 2)
        return (remote(sums.at[q, a_give, :], in2.at[r, 0], s2.at[0, j], r2.at[0, j], me.x_dev),
                remote(sums.at[q, b_give, :], in2.at[r, 1], s2.at[1, j], r2.at[1, j], me.y_dev))

    def c3(j):
        q, r = room(j), lax.rem(j, 2)
        return (remote(sums.at[q, a_pass, :], in3.at[r, 0], s3.at[0, j], r3.at[0, j], me.y_dev),
                remote(sums.at[q, b_pass, :], in3.at[r, 1], s3.at[1, j], r3.at[1, j], me.x_dev))

    def c4(j, ref, a_rows, b_rows):
        q, dst = room(j), ref.at[layers - 1 - lax.div(j, 2)]
        return (remote(sums.at[q, a_rows, :], dst.at[a_rows, :], s4.at[0, j], r4.at[0, j], me.y_dev),
                remote(sums.at[q, b_rows, :], dst.at[b_rows, :], s4.at[1, j], r4.at[1, j], me.x_dev))

    def keep(j, ref):
        q, dst = room(j), ref.at[layers - 1 - lax.div(j, 2)]
        return (pltpu.make_async_copy(sums.at[q, a_last, :], dst.at[a_last, :], out_sem.at[0, lax.rem(j, 2)]),
                pltpu.make_async_copy(sums.at[q, b_last, :], dst.at[b_last, :], out_sem.at[1, lax.rem(j, 2)]))

    def c5(j, ref, a_rows, b_rows):
        dst = ref.at[layers - 1 - lax.div(j, 2)]
        return (remote(dst.at[a_rows, :], dst.at[a_rows, :], s5.at[0, j], r5.at[0, j], me.x_dev),
                remote(dst.at[b_rows, :], dst.at[b_rows, :], s5.at[1, j], r5.at[1, j], me.y_dev))

    def c6(j, ref, which):
        dst = ref.at[layers - 1 - lax.div(j, 2)]
        return remote(dst.at[which, :], dst.at[which, :], s6.at[j], r6.at[j], me.partner)

    def add(j, start, size, buffer):
        q = room(j)
        step = min(32, size)

        def body(i, carry):
            there = pl.ds(pl.multiple_of(start + i * step, step), step)
            sums[q, there, :] = sums[q, there, :] + buffer[pl.ds(pl.multiple_of(i * step, step), step), :]
            return carry

        lax.fori_loop(0, size // step, body, 0)

    def step1(j):
        @pl.when(j >= 2)
        def _():
            pl.semaphore_wait(free1, 1)

        c1(j).start()

    def step2(j):
        c1(j).wait_recv()
        add(j, own, hd, in1.at[lax.rem(j, 2)])

        @pl.when(j < 2 * layers - 2)
        def _():
            pl.semaphore_signal(free1, inc=1, device_id=me.partner, device_id_type=MESH)

        for copy in c2(j):
            copy.start()

    def step3(j):
        r, got, put = lax.rem(j, 2), c2(j), c3(j)
        for k, start in enumerate((a_base + me.x * e8, b_base + me.y * e8)):
            got[k].wait_recv()
            add(j, start, e8, in2.at[r, k])
            put[k].start()

    def step4(j, ref):
        r, got, put, local = lax.rem(j, 2), c3(j), c4(j, ref, a_last, b_last), keep(j, ref)
        for k, start in enumerate((a_base + me.x * e8 + me.y * e16, b_base + me.y * e8 + me.x * e16)):
            got[k].wait_recv()
            add(j, start, e16, in3.at[r, k])
            put[k].start()
            local[k].start()

    def step5(j, ref):
        got, put, local = c4(j, ref, a_pass, b_pass), c5(j, ref, a_keep, b_keep), keep(j, ref)
        for k in (0, 1):
            local[k].wait()
            got[k].wait_recv()
            put[k].start()

    def step6(j, ref):
        for copy in c5(j, ref, a_give, b_give):
            copy.wait_recv()
        c6(j, ref, own_rows).start()

    def step7(j, ref):
        c6(j, ref, other_rows).wait_recv()

    def settle(j, ref):
        c1(j).wait_send()
        for copy in c2(j) + c3(j) + c4(j, ref, a_last, b_last):
            copy.wait_send()

    def finish(j, ref):
        for copy in c5(j, ref, a_keep, b_keep):
            copy.wait_send()
        c6(j, ref, own_rows).wait_send()

    def run(k, j):
        ref = gd_ref if j % 2 == 0 else gu_ref
        (step1, step2, step3, step4, step5, step6, step7)[k - 1](*((j,) if k <= 3 else (j, ref)))

    def at_place(tau, p, steps):
        at_step(plan, 32 * tau + p, 32, steps, run)

    def u_copy(n):
        l, s, t, slot = layers - 1 - lax.div(n, 4 * TILES), lax.rem(lax.div(n, TILES), 4), lax.rem(n, TILES), lax.rem(n, 2)
        return pltpu.make_async_copy(u_ref.at[4 * l + s, pl.ds(t * tm, tm), :], u_v.at[slot], u_sem.at[slot])

    def load_h(l):
        @pl.when(l == 0)
        def _():
            pltpu.make_async_copy(x_ref, h_v, h_sem).start()

        @pl.when(l > 0)
        def _():
            pltpu.make_async_copy(h_ref.at[l - 1], h_v, h_sem).start()

    def wait_w(i):
        for k in (0, 1):
            pltpu.make_async_copy(up_ref.at[0], w_v.at[lax.rem(i, 2), k], w_sem.at[lax.rem(i, 2), k]).wait()

    def next_g():
        step = min(64, m)

        def body(i, carry):
            here = pl.ds(pl.multiple_of(i * step, step), step)
            g_v[here, :] = acc_v[here, :].astype(BF16)
            acc_v[here, :] = g_v[here, :].astype(F32)
            return carry

        lax.fori_loop(0, m // step, body, 0)

    load_h(layers - 1)
    u_copy(0).start()
    tiles_total = TILES * (4 * (layers - 1) + 1)
    groups = 4 * (layers - 1) + 1

    def layer(tau, carry):
        l = layers - 1 - tau
        down, up = 2 * tau, 2 * tau + 1
        room_down, room_up = room(down), room(up)
        load_a(l).wait()

        @pl.when(tau > 0)
        def _():
            settle(down - 2, gd_ref)

        def product(room_j, lhs, rhs, base):
            def body(i, carry):
                cols = at(lax.rem(i + 1 + me.core, 2) * broad, broad)
                sums[room_j, cols, :] = dot_rows(lhs[:, cols], rhs[...])
                at_place(tau, base + i, (base, base + 1))
                return carry

            lax.fori_loop(0, 2, body, 0)

        product(room_down, a_v, g_v, 0)

        @pl.when(l > 0)
        def _():
            load_a(l - 1).start()

        def step(n, carry):
            k = 4 * TILES * tau + n
            block, slot = 4 * tau + lax.div(n, TILES), lax.rem(k, 2)
            ws = lax.rem(block, 2)
            here = pl.ds(pl.multiple_of(lax.rem(n, TILES) * tm, tm), tm)

            @pl.when(k + 1 < tiles_total)
            def _():
                u_copy(k + 1).start()

            @pl.when(lax.rem(n, TILES) == 0)
            def _():
                @pl.when(block + 1 < groups)
                def _():
                    load_w(block + 1)

                wait_w(block)

            u_copy(k).wait()
            few = tm // PARTS_BACKWARD
            for r in range(0, tm, few):
                some = pl.ds(pl.multiple_of(lax.rem(n, TILES) * tm + r, few), few)
                for j in range(0, d, wide):
                    da = dot_cols(g_v[some, :], w_v[ws, 1, j:j + wide, :])
                    v = u_v[slot, r:r + few, j:j + wide].astype(F32)
                    v2 = v * v
                    th = jnp.tanh(v * (K0 + K1 * v2))
                    slope = (1.0 + th) * (0.5 + (v * (1.0 - th)) * ((0.5 * K0) + (1.5 * K1) * v2))
                    d_v[some, j:j + wide] = (da * slope).astype(BF16)
            place = 2 * n + jnp.where(n >= TILES, 4, 2)
            at_place(tau, place, [2, 4] + list(range(8, 20, 2)))

            @pl.when(l > 0)
            def _():
                for j in range(0, d, wide):
                    acc_v[here, j:j + wide] += dot_cols(d_v[here, :], w_v[ws, 0, j:j + wide, :])

            at_place(tau, place + 1, [3, 5] + list(range(9, 20, 2)))

            @pl.when(n == TILES - 1)
            def _():
                pltpu.make_async_copy(x_ref, h_v, h_sem).wait()

                @pl.when(tau >= 2)
                def _():
                    settle(up - 4, gu_ref)

                product(room_up, h_v, d_v, 6)

                @pl.when(l > 0)
                def _():
                    load_h(l - 1)

            return carry

        lax.fori_loop(0, jnp.where(l > 0, 4 * TILES, TILES), step, 0)

        @pl.when(l > 0)
        def _():
            next_g()
            at_place(tau, 20, (20,))

        return carry

    lax.fori_loop(0, layers, layer, 0)
    for p, k, j in plan:
        if p >= 32 * layers:
            run(k, j)
    for j in range(2 * layers):
        ref = gd_ref if j % 2 == 0 else gu_ref
        finish(j, ref)
        if j >= 2 * layers - 3 and j != 2 * layers - 4:
            settle(j, ref)


def kernel(
    layers, total, x_ref, t_ref, up_ref, down_ref, w_ref, u_ref, a_ref, h_ref, gu_ref, gd_ref,
    h_v, y_v, t_v, w_v, u_v, act_v, d_v, a_v, sums, in1, in2, in3,
    w_sem, u_sem, act_sem, h_sem, t_sem, back_u_sem, back_a_sem, back_h_sem, out_sem, free1, *sems,
):
    def load_a(l):
        return pltpu.make_async_copy(a_ref.at[l], a_v, back_a_sem)

    def load_w(i):
        l, s = layers - 1 - lax.div(i, 4), lax.rem(i, 4)
        ws = lax.rem(i, 2)

        @pl.when(s == 0)
        def _():
            pltpu.make_async_copy(up_ref.at[l], w_v.at[ws, 0], w_sem.at[ws, 0]).start()
            pltpu.make_async_copy(down_ref.at[l], w_v.at[ws, 1], w_sem.at[ws, 1]).start()

        @pl.when(s > 0)
        def _():
            c = 3 * l + s - 1
            for k in (0, 1):
                pltpu.make_async_copy(w_ref.at[c, k], w_v.at[ws, k], w_sem.at[ws, k]).start()

    def prefetch():
        load_a(layers - 1).start()
        load_w(0)

    drain = forward_pass(
        layers, total, prefetch, x_ref, t_ref, up_ref, down_ref, w_ref, u_ref, a_ref, h_ref,
        h_v, y_v, t_v, w_v, u_v, act_v, w_sem, u_sem, act_sem, h_sem, t_sem, *sems[:16],
    )
    backward_pass(
        layers, load_a, load_w, x_ref, h_ref, up_ref, u_ref, gu_ref, gd_ref,
        h_v, y_v, w_v, u_v, d_v, a_v, t_v, sums, in1, in2, in3,
        w_sem, back_u_sem, back_h_sem, out_sem, free1, *sems[16:],
    )
    drain()


def any_specs(count):
    return [pl.BlockSpec(memory_space=pl.ANY)] * count


def local_step(hidden, targets, w_up, w_down, total_tokens):
    layers, d, own = w_up.shape
    m = hidden.shape[0]
    tm = m // TILES
    groups = 3 * layers
    dma = pltpu.SemaphoreType.DMA
    out = pl.pallas_call(
        functools.partial(kernel, layers, float(total_tokens)),
        out_shape=[
            jax.ShapeDtypeStruct((groups, 2, d, own), BF16),
            jax.ShapeDtypeStruct((4 * layers, m, own), BF16),
            jax.ShapeDtypeStruct((layers, m, own), BF16),
            jax.ShapeDtypeStruct((layers - 1, m, d), BF16),
            jax.ShapeDtypeStruct((layers, d, own), F32),
            jax.ShapeDtypeStruct((layers, own, d), F32),
        ],
        in_specs=any_specs(4),
        out_specs=any_specs(6),
        scratch_shapes=[
            pltpu.VMEM((m, d), BF16),
            pltpu.VMEM((m, d), F32),
            pltpu.VMEM((m, d), BF16),
            pltpu.VMEM((2, 2, d, own), BF16),
            pltpu.VMEM((2, tm, own), BF16),
            pltpu.VMEM((2, tm, own), BF16),
            pltpu.VMEM((m, own), BF16),
            pltpu.VMEM((m, own), BF16),
            pltpu.VMEM((3, d, own), F32),
            pltpu.VMEM((2, d // 2, own), F32),
            pltpu.VMEM((2, 2, d // 8, own), F32),
            pltpu.VMEM((2, 2, d // 16, own), F32),
            dma((2, 2)), dma((2,)), dma((2,)), dma((TILES,)), dma((2,)),
            dma((2,)), dma, dma, dma((2, 2)), pltpu.SemaphoreType.REGULAR,
        ] + [dma((groups,))] * 16 + [dma((2 * layers,))] * 2 + [dma((2, 2 * layers))] * 8 + [dma((2 * layers,))] * 2,
        compiler_params=pltpu.CompilerParams(collective_id=0, has_side_effects=True, vmem_limit_bytes=66_900_000),
        name="gradients",
    )(hidden, targets, w_up, w_down)
    return out[4], out[5]


def solution(mesh):
    def grad_step(hidden_in, targets, w_up, w_down):
        step_fn = functools.partial(local_step, total_tokens=hidden_in.shape[0])
        mapped = jax.shard_map(step_fn, mesh=mesh, in_specs=(P("dp", None), P("dp", None), P(None, None, "tp"), P(None, "tp", None)), out_specs=(P(None, None, "tp"), P(None, "tp", None)), check_vma=False)
        return mapped(hidden_in, targets, w_up, w_down)

    return grad_step
```
